256 devices in a mesh: rows: 32 (over y, x, core), feat: 8 (over z).
Axes of the slice: x: 4, y: 4, z: 8, core: 2. Of those that a mesh axis runs over, the one named last changes fastest.
Arguments:
- features: bfloat16 [32768, 2048], P('rows', 'feat'), may hold values from -6 to 6
- grad_out: bfloat16 [32768, 2048], P('rows', 'feat'), may hold values from -6 to 6
- eigvecs: float32 [2048, 2048], P('feat', 'rows'), may hold values from -1 to 1, as said below
- eigvals: float32 [2048], replicated, may hold values from 0.1 to 1, as said below
- whiten: bfloat16 [2048, 2048], P(None, 'feat'), may hold values from -0.125 to 0.125
Outputs:
- grad_in: bfloat16 [32768, 2048], P('rows', 'feat')
The draws below stay inside these ranges and needn't reach their ends.
Inputs may be any that keep to these rules, and one draw needn't show every extreme that they name: `eigvecs`: the columns are orthonormal. `eigvals`: any two entries differ by at least 0.45 / 2048.
All inputs are finite; a program needn't handle non-finite values.
Results may differ from the reference program's by a relative error of at most 0.0074.
Values may be sent and summed in bfloat16 or wider, within the bound.
A program may use at most 128 MiB of HBM per device.

```python
import jax
import jax.numpy as jnp
from jax import lax

D = 2048
TOKENS = 32768


def draw_eigvecs(key, part):
    normal_mat = jax.random.normal(key, (D, D), jnp.float32)
    ortho, upper = jnp.linalg.qr(normal_mat)
    return ortho


def draw_eigvals(key, part):
    ranking = jax.random.permutation(jax.random.fold_in(key, 1), D)
    jitter = jax.random.uniform(jax.random.fold_in(key, 2), (D,), jnp.float32)
    return 0.1 + 0.9 * (ranking.astype(jnp.float32) + 0.25 + 0.5 * jitter) / D


def block_levels(own_key, extent, shards, low, top_value):
    loudness, own = 1.0, jax.random.fold_in(own_key, 6)
    for dim, parts in shards:
        heights = jnp.exp(jax.random.uniform(jax.random.fold_in(own, dim), (parts,), jnp.float32, low / len(shards), top_value / len(shards)))
        loudness = loudness * jnp.repeat(heights, extent[dim] // parts).reshape([-1 if axis == dim else 1 for axis in range(len(extent))])
    return loudness


def gaussian(own_key, extent, width, bound, split=(), held_as=jnp.bfloat16):
    entries = width * jax.random.normal(own_key, extent, jnp.float32)
    if split:
        entries = entries * block_levels(own_key, extent, split, -0.22, 0.18)
    return jnp.clip(entries, -bound, bound).astype(held_as)


def setup_inputs(seed: int = 0) -> dict:
    keys = jax.random.split(jax.random.key(seed), 6)
    return {
        "features": gaussian(keys[0], (TOKENS, D), 1.0, 6.0, ((0, 32), (1, 8))),
        "grad_out": gaussian(keys[1], (TOKENS, D), 1.0, 6.0, ((0, 32), (1, 8))),
        "eigvecs": draw_eigvecs(jax.random.fold_in(keys[5], 71), 0),
        "eigvals": draw_eigvals(jax.random.fold_in(keys[5], 71), 0),
        "whiten": gaussian(keys[4], (D, D), D ** -0.5, 0.125, ((1, 8),)),
    }


def divided(lam_row, lam_col, first_col):
    on_diag = jnp.arange(lam_row.shape[0], dtype=jnp.int32)[:, None] == (first_col + jnp.arange(lam_col.shape[0], dtype=jnp.int32))[None, :]
    root_row = lam_row ** (-0.5)
    root_col = lam_col ** (-0.5)
    gaps_lam = lam_row[:, None] - lam_col[None, :]
    safe_gap = jnp.where(on_diag, jnp.ones_like(gaps_lam), gaps_lam)
    off_diag = (root_row[:, None] - root_col[None, :]) / safe_gap
    diag_vals = -0.5 * lam_row[:, None] ** (-1.5) + jnp.zeros_like(gaps_lam)
    return jnp.where(on_diag, diag_vals, off_diag)

def reference(features, grad_out, eigvecs, eigvals, whiten):
    highest = lax.Precision.HIGHEST
    row_count = features.shape[0]
    col_mean = jnp.sum(features.astype(jnp.float32), axis=0) / row_count
    grad_mean = jnp.sum(grad_out.astype(jnp.float32), axis=0) / row_count
    cross_prod = jnp.dot(features.T.astype(jnp.float32), grad_out.astype(jnp.float32), preferred_element_type=jnp.float32) - row_count * jnp.outer(col_mean, grad_mean)
    sym_gram = 0.5 * (cross_prod + cross_prod.T)
    rotated = jnp.dot(eigvecs.T, jnp.dot(sym_gram, eigvecs, precision=highest), precision=highest)
    kernel = divided(eigvals, eigvals, 0)
    sens = jnp.dot(jnp.dot(eigvecs, kernel * rotated, precision=highest), eigvecs.T, precision=highest)
    sens_scaled = (2.0 / row_count * sens).astype(jnp.bfloat16)
    shifted = (grad_out.astype(jnp.float32) - grad_mean).astype(jnp.bfloat16)
    centered = (features.astype(jnp.float32) - col_mean).astype(jnp.bfloat16)
    grad_in = jnp.dot(shifted.astype(jnp.float32), whiten.astype(jnp.float32), preferred_element_type=jnp.float32) + jnp.dot(centered.astype(jnp.float32), sens_scaled.T.astype(jnp.float32), preferred_element_type=jnp.float32)
    return grad_in.astype(jnp.bfloat16)
```

```python
import functools

import jax
import jax.numpy as jnp
from jax import lax
from jax.experimental import pallas as pl
from jax.experimental.pallas import tpu as pltpu
from jax.sharding import PartitionSpec as P

MESH = pl.DeviceIdType.MESH
F32 = jnp.float32
BF16 = jnp.bfloat16
VMEM_CAP = 60 * 1024 * 1024


class Dims:
    def __init__(self, rows, feat, tokens, d):
        self.nr, self.nz = rows, feat
        self.nk = rows // 2
        self.nx = {4: 2, 16: 4}[self.nk]
        self.ny = self.nk // self.nx
        self.kh = self.nk // 2
        self.d, self.dh = d, d // 2
        self.n = tokens
        self.tok = tokens // rows
        self.fb = d // feat
        self.fbh = self.fb // 2
        self.sr = self.fb // self.nk
        self.ea = d // self.nk
        self.er = d // rows


def where_am_i(s):
    r = lax.axis_index("rows")
    z = lax.axis_index("feat")
    return r, z, r // 2, lax.rem(r, 2)


def send(src, dst, ss, rs, r, z):
    copy = pltpu.make_async_remote_copy(
        src, dst, ss, rs, device_id={"rows": r, "feat": z}, device_id_type=MESH
    )
    copy.start()


def arrive(ref, sem):
    pltpu.make_async_copy(ref, ref, sem).wait()


def greet(s, r, z):
    barrier = pltpu.get_barrier_semaphore()

    def plane(t, _):
        pl.semaphore_signal(
            barrier, 1, device_id={"rows": lax.rem(r + t, s.nr), "feat": z}, device_id_type=MESH
        )
        return 0

    def line(t, _):
        pl.semaphore_signal(
            barrier, 1, device_id={"rows": r, "feat": lax.rem(z + t, s.nz)}, device_id_type=MESH
        )
        return 0

    lax.fori_loop(1, s.nr, plane, 0)
    lax.fori_loop(1, s.nz, line, 0)
    pl.semaphore_wait(barrier, s.nr - 1 + s.nz - 1)


def basis_kernel(
    s, x_ref, g_ref, v_ref, vh_ref, mean_ref, xc_ref, xct_ref,
    pad, pad_in, tile, grid, m_out, m_in, ssem, rsem, p2sem, lsem,
):
    r, z, k, c = where_am_i(s)
    y, x = k // s.nx, lax.rem(k, s.nx)
    mate = r + 1 - 2 * c
    first = c == 0
    a = jnp.where(first, x, y)
    b = jnp.where(first, y, x)

    v = v_ref[...]
    twice = jnp.concatenate([v, v], axis=1)
    lane_half = lax.broadcasted_iota(jnp.int32, twice.shape, 1) // s.er
    pad[...] = jnp.where(lane_half == c, twice, 0.0).astype(BF16)
    sum_x = jnp.sum(x_ref[...].astype(F32), axis=0, keepdims=True)
    sum_g = jnp.sum(g_ref[...].astype(F32), axis=0, keepdims=True)
    m_out[0] = jnp.concatenate([sum_x, sum_g], axis=1)
    m_in[r] = m_out[0]

    greet(s, r, z)

    send(pad, pad_in, ssem.at[0], rsem.at[0], mate, z)

    def sums(t, _):
        send(m_out.at[0], m_in.at[r], ssem.at[1], rsem.at[1], lax.rem(r + t, s.nr), z)
        return 0

    lax.fori_loop(1, s.nr, sums, 0)
    arrive(pad_in, rsem.at[0])
    tile[...] = pad[...] + pad_in[...]
    grid[b, a, z] = tile[pl.ds(pl.multiple_of(c * s.fbh, s.fbh), s.fbh), :]

    def up(t, _):
        send(grid.at[b, a, z], grid.at[b, a, z], ssem.at[2], rsem.at[2], r, lax.rem(z + t, s.nz))
        return 0

    lax.fori_loop(1, s.nz, up, 0)

    arrive(m_in.at[pl.ds(0, s.nr - 1)], rsem.at[1])
    mean = jnp.sum(m_in[...], axis=0) / s.n
    mean_ref[z] = mean

    def mean_up(t, _):
        send(mean_ref.at[z], mean_ref.at[z], ssem.at[3], rsem.at[3], r, lax.rem(z + t, s.nz))
        return 0

    lax.fori_loop(1, s.nz, mean_up, 0)
    centered = (x_ref[...].astype(F32) - mean[:, : s.fb]).astype(BF16)
    xc_ref[...] = centered
    xct_ref[...] = centered.astype(F32).T.astype(BF16)

    arrive(grid.at[0, 0, pl.ds(0, s.nz - 1)], rsem.at[2])

    def along_a(t, _):
        a2 = lax.rem(a + t, s.nx)
        y2, x2 = jnp.where(first, y, a2), jnp.where(first, a2, x)
        send(grid.at[b, a], grid.at[b, a], ssem.at[4], rsem.at[4], (y2 * s.nx + x2) * 2 + c, z)
        return 0

    lax.fori_loop(1, s.nx, along_a, 0)
    arrive(grid.at[0, pl.ds(0, s.nx - 1)], rsem.at[4])

    def along_b(t, _):
        b2 = lax.rem(b + t, s.ny)
        y2, x2 = jnp.where(first, b2, y), jnp.where(first, x, b2)
        send(grid.at[b], grid.at[b], ssem.at[5], p2sem.at[t], (y2 * s.nx + x2) * 2 + c, z)
        return 0

    lax.fori_loop(1, s.ny, along_b, 0)

    def hand_out(b2):
        def each(a2, _):
            y2, x2 = jnp.where(first, b2, a2), jnp.where(first, a2, b2)
            half = y2 // (s.ny // 2)
            kk = lax.rem(y2, s.ny // 2) * s.nx + x2
            cols = pl.ds(pl.multiple_of(kk * s.ea, s.ea), s.ea)
            dst = vh_ref.at[:, c, :, cols]

            @pl.when(half == c)
            def _():
                pltpu.make_async_copy(grid.at[b2, a2], dst, lsem).start()

            @pl.when(half != c)
            def _():
                send(grid.at[b2, a2], dst, ssem.at[6], rsem.at[6], mate, z)

            return 0

        lax.fori_loop(0, s.nx, each, 0)

    hand_out(b)

    def landed(t, _):
        b2 = lax.rem(b + s.ny - t, s.ny)
        arrive(grid.at[b2], p2sem.at[t])
        hand_out(b2)
        return 0

    lax.fori_loop(1, s.ny, landed, 0)

    arrive(mean_ref.at[pl.ds(0, s.nz - 1)], rsem.at[3])
    arrive(vh_ref.at[:, c], lsem)
    arrive(vh_ref.at[:, 1 - c], rsem.at[6])
    arrive(pad, ssem.at[0])
    arrive(m_in.at[pl.ds(0, s.nr - 1)], ssem.at[1])
    arrive(grid.at[0, 0, pl.ds(0, s.nz - 1)], ssem.at[2])
    arrive(mean_ref.at[pl.ds(0, s.nz - 1)], ssem.at[3])
    arrive(grid.at[0, pl.ds(0, s.nx - 1)], ssem.at[4])
    arrive(grid.at[pl.ds(0, s.ny - 1)], ssem.at[5])
    arrive(vh_ref.at[:, c], ssem.at[6])


def eigen_kernel(
    s, xct_ref, g_ref, vh_ref, mean_ref, kk_ref, w_ref, acc_ref, sens_ref,
    vv, cp, cp_in, part, part_in, c128, t1s, t1r, mt, sy_out, sy_in, t2p, t2d, t2s, t2g,
    sp, sp_out, sp_in, ssem, rsem, lsem,
):
    r, z, k, c = where_am_i(s)
    mate = r + 1 - 2 * c
    half = k // s.kh
    mine = half == c
    kk = lax.rem(k, s.kh)
    nzh = s.nz // 2

    load_v = pltpu.make_async_copy(vh_ref, vv, lsem)
    load_v.start()
    col_sum = jnp.sum(xct_ref[...].astype(F32), axis=1, keepdims=True)

    def gram(block):
        prod = jnp.dot(xct_ref[...], g_ref[block], preferred_element_type=F32)
        nu = mean_ref[block][:, s.fb :]
        return prod - col_sum * nu

    def cols_of(q):
        return pl.ds(pl.multiple_of(q * s.fb, s.fb), s.fb)

    def gram_theirs(q, _):
        cp[1, :, cols_of(q)] = gram((1 - c) * nzh + q)
        return 0

    lax.fori_loop(0, nzh, gram_theirs, 0)
    greet(s, r, z)
    send(cp.at[1], cp_in, ssem.at[0], rsem.at[0], mate, z)

    def gram_ours(q, _):
        cp[0, :, cols_of(q)] = gram(c * nzh + q)
        return 0

    lax.fori_loop(0, nzh, gram_ours, 0)
    arrive(cp_in, rsem.at[0])

    def slab(j, _):
        rows = pl.ds(pl.multiple_of(j * s.sr, s.sr), s.sr)
        part[j] = (cp[0, rows, :] + cp_in[rows, :]).astype(BF16)
        return 0

    lax.fori_loop(0, s.nk, slab, 0)

    def scatter(t, _):
        k2 = lax.rem(k + t, s.nk)
        send(part.at[k2], part_in.at[k], ssem.at[1], rsem.at[1], 2 * k2 + c, z)
        return 0

    lax.fori_loop(1, s.nk, scatter, 0)
    part_in[k] = part[k]

    acc_ref[...] = jnp.zeros_like(acc_ref)

    def product(q, _):
        nu = mean_ref[q][:, s.fb :]
        shifted = (g_ref[q].astype(F32) - nu).astype(BF16)
        acc_ref[...] += jnp.dot(shifted, w_ref[q], preferred_element_type=F32)
        return 0

    lax.fori_loop(0, s.nz, product, 0)

    arrive(part_in.at[pl.ds(0, s.nk - 1)], rsem.at[1])
    c128[c, z] = jnp.sum(part_in[...].astype(F32), axis=0).astype(BF16)

    def up(t, _):
        send(c128.at[c, z], c128.at[c, z], ssem.at[2], rsem.at[2], r, lax.rem(z + t, s.nz))
        return 0

    lax.fori_loop(1, s.nz, up, 0)
    load_v.wait()
    arrive(c128.at[c, pl.ds(0, s.nz - 1)], rsem.at[2])
    send(c128.at[c], c128.at[c], ssem.at[3], rsem.at[3], mate, z)

    def basis_rows(h):
        return vv[pl.ds(h * nzh, nzh)].reshape(s.dh, s.dh)

    t1 = jnp.dot(c128[c].reshape(s.ea, s.dh), basis_rows(c), preferred_element_type=F32)
    arrive(c128.at[1 - c], rsem.at[3])
    t1 += jnp.dot(c128[1 - c].reshape(s.ea, s.dh), basis_rows(1 - c), preferred_element_type=F32)
    for j in range(s.kh):
        t1s[j] = t1[:, j * s.ea : (j + 1) * s.ea].astype(BF16).reshape(s.nz, s.sr, s.ea)

    def turn(t, _):
        j = lax.rem(kk + t, s.kh)
        k2 = c * s.kh + j

        @pl.when(k2 != k)
        def _():
            send(t1s.at[j], t1r.at[:, k], ssem.at[4], rsem.at[4], 2 * k2 + c, z)

        send(t1s.at[j], t1r.at[:, k], ssem.at[5], rsem.at[4], 2 * k2 + 1 - c, z)
        return 0

    lax.fori_loop(0, s.kh, turn, 0)

    @pl.when(mine)
    def _():
        t1r[:, k] = t1s[kk]
        arrive(t1r.at[:, pl.ds(0, s.nk - 1)], rsem.at[4])
        arrive(t1s.at[pl.ds(0, s.kh - 1)], ssem.at[4])

    @pl.when(jnp.logical_not(mine))
    def _():
        arrive(t1r, rsem.at[4])
        arrive(t1s, ssem.at[4])

    arrive(t1s, ssem.at[5])

    left = t1r[...].reshape(s.d, s.ea).astype(F32).T.astype(BF16)
    mt[...] = jnp.dot(left, vv[...].reshape(s.d, s.dh), preferred_element_type=F32)
    for j in range(s.kh):
        sy_out[j] = mt[:, j * s.ea : (j + 1) * s.ea].T.astype(BF16)

    def mirror(t, _):
        j = lax.rem(kk + t, s.kh)
        k2 = c * s.kh + j

        @pl.when(k2 != k)
        def _():
            send(sy_out.at[j], sy_in.at[kk], ssem.at[6], rsem.at[6], 2 * k2 + half, z)

        return 0

    lax.fori_loop(0, s.kh, mirror, 0)

    @pl.when(mine)
    def _():
        sy_in[kk] = sy_out[kk]
        arrive(sy_in.at[pl.ds(0, s.kh - 1)], rsem.at[6])
        arrive(sy_out.at[pl.ds(0, s.kh - 1)], ssem.at[6])

    @pl.when(jnp.logical_not(mine))
    def _():
        arrive(sy_in, rsem.at[6])
        arrive(sy_out, ssem.at[6])

    total = jnp.zeros((s.ea, s.fb), F32)
    own_rows = vv.at[z]
    for j in range(s.kh):
        cols = slice(j * s.ea, (j + 1) * s.ea)
        rotated = 0.5 * (mt[:, cols] + sy_in[j].astype(F32))
        weighted = (kk_ref[:, cols] * rotated).astype(BF16)
        right = own_rows[:, :, cols].reshape(s.fb, s.ea)
        total += lax.dot_general(
            weighted, right, (((1,), (1,)), ((), ())), preferred_element_type=F32
        )
    t2p[...] = total
    send(t2p, t2d, ssem.at[7], rsem.at[7], mate, z)
    arrive(t2d, rsem.at[7])
    t2s[...] = (t2p[...] + t2d[...]).astype(BF16).reshape(t2s.shape)

    def spread(t, _):
        k2 = lax.rem(k + t, s.nk)
        send(t2s.at[c], t2g.at[kk, c], ssem.at[8], rsem.at[8], 2 * k2 + half, z)
        return 0

    lax.fori_loop(1, s.nk, spread, 0)

    @pl.when(mine)
    def _():
        t2g[kk] = t2s[...]
        arrive(t2g.at[pl.ds(0, s.kh - 1)], rsem.at[8])

    @pl.when(jnp.logical_not(mine))
    def _():
        arrive(t2g, rsem.at[8])

    right2 = t2g[...].reshape(s.dh, s.fb)

    def back(q, _):
        prod = jnp.dot(vv[q].reshape(s.fb, s.dh), right2, preferred_element_type=F32)
        prod = prod * (2.0 / s.n)
        sp[q] = prod
        sp_out[q] = prod.astype(BF16)
        send(sp_out.at[q], sp_in.at[q], ssem.at[9], rsem.at[9], mate, z)
        return 0

    lax.fori_loop(0, s.nz, back, 0)
    arrive(sp_in, rsem.at[9])

    def finish(q, _):
        sens_ref[q] = (sp[q] + sp_in[q].astype(F32)).astype(BF16)
        return 0

    lax.fori_loop(0, s.nz, finish, 0)

    arrive(cp_in, ssem.at[0])
    arrive(part.at[pl.ds(0, s.nk - 1)], ssem.at[1])
    arrive(c128.at[c, pl.ds(0, s.nz - 1)], ssem.at[2])
    arrive(c128.at[c], ssem.at[3])
    arrive(t2p, ssem.at[7])
    arrive(part.at[pl.ds(0, s.nk - 1)], ssem.at[8])
    arrive(sp_out, ssem.at[9])


def final_kernel(acc_ref, x_ref, sens_ref, out_ref, total):
    q = pl.program_id(0)

    @pl.when(q == 0)
    def _():
        total[...] = acc_ref[...]

    total[...] += jnp.dot(x_ref[0], sens_ref[0], preferred_element_type=F32)

    @pl.when(q == pl.num_programs(0) - 1)
    def _():
        out_ref[...] = total[...].astype(BF16)


def vm():
    return pl.BlockSpec(memory_space=pltpu.VMEM)


def anywhere():
    return pl.BlockSpec(memory_space=pl.ANY)


def local(features, grad_out, eigvecs, eigvals, whiten):
    tok, fb = features.shape
    s = Dims(lax.axis_size("rows"), lax.axis_size("feat"), tok * lax.axis_size("rows"), whiten.shape[0])
    sd = jax.ShapeDtypeStruct
    dma = pltpu.SemaphoreType.DMA

    grad_all = lax.all_gather(grad_out, "feat", axis=0, tiled=False)

    vh, means, centered, centered_t = pl.pallas_call(
        functools.partial(basis_kernel, s),
        name="basis",
        out_shape=(
            sd((s.nz, 2, s.fbh, s.dh), BF16),
            sd((s.nz, 1, 2 * s.fb), F32),
            sd((tok, fb), BF16),
            sd((fb, tok), BF16),
        ),
        in_specs=[vm(), vm(), vm()],
        out_specs=(anywhere(), vm(), vm(), vm()),
        scratch_shapes=[
            pltpu.VMEM((s.fb, s.ea), BF16),
            pltpu.VMEM((s.fb, s.ea), BF16),
            pltpu.VMEM((s.fb, s.ea), BF16),
            pltpu.VMEM((s.ny, s.nx, s.nz, s.fbh, s.ea), BF16),
            pltpu.VMEM((1, 1, 2 * s.fb), F32),
            pltpu.VMEM((s.nr, 1, 2 * s.fb), F32),
            dma((7,)),
            dma((7,)),
            dma((s.ny,)),
            dma,
        ],
        compiler_params=pltpu.CompilerParams(
            collective_id=0, has_side_effects=True, vmem_limit_bytes=VMEM_CAP
        ),
        cost_estimate=pl.CostEstimate(flops=40_000_000_000, bytes_accessed=16_000_000, transcendentals=0),
    )(features, grad_out, eigvecs)

    centered_all = lax.all_gather(centered, "feat", axis=0, tiled=False)

    r = lax.axis_index("rows")
    k, c = r // 2, lax.rem(r, 2)
    root = eigvals ** (-0.5)
    s_row = lax.dynamic_slice_in_dim(root, k * s.ea, s.ea)[:, None]
    s_col = lax.dynamic_slice_in_dim(root, c * s.dh, s.dh)[None, :]
    both = s_row * s_col
    weights = -(both * both) / (s_row + s_col)

    acc, sens = pl.pallas_call(
        functools.partial(eigen_kernel, s),
        name="eigen",
        out_shape=(sd((tok, fb), F32), sd((s.nz, s.fb, s.fb), BF16)),
        in_specs=[vm(), vm(), anywhere(), vm(), vm(), vm()],
        out_specs=(vm(), vm()),
        scratch_shapes=[
            pltpu.VMEM((s.nz, 2, s.fbh, s.dh), BF16),
            pltpu.VMEM((2, s.fb, s.dh), F32),
            pltpu.VMEM((s.fb, s.dh), F32),
            pltpu.VMEM((s.nk, s.sr, s.dh), BF16),
            pltpu.VMEM((s.nk, s.sr, s.dh), BF16),
            pltpu.VMEM((2, s.nz, s.sr, s.dh), BF16),
            pltpu.VMEM((s.kh, s.nz, s.sr, s.ea), BF16),
            pltpu.VMEM((s.nz, s.nk, s.sr, s.ea), BF16),
            pltpu.VMEM((s.ea, s.dh), F32),
            pltpu.VMEM((s.kh, s.ea, s.ea), BF16),
            pltpu.VMEM((s.kh, s.ea, s.ea), BF16),
            pltpu.VMEM((s.ea, s.fb), F32),
            pltpu.VMEM((s.ea, s.fb), F32),
            pltpu.VMEM((2, s.ea // 2, s.fb), BF16),
            pltpu.VMEM((s.kh, 2, s.ea // 2, s.fb), BF16),
            pltpu.VMEM((s.nz, s.fb, s.fb), F32),
            pltpu.VMEM((s.nz, s.fb, s.fb), BF16),
            pltpu.VMEM((s.nz, s.fb, s.fb), BF16),
            dma((10,)),
            dma((10,)),
            dma,
        ],
        compiler_params=pltpu.CompilerParams(
            collective_id=1, has_side_effects=True, vmem_limit_bytes=VMEM_CAP
        ),
        cost_estimate=pl.CostEstimate(flops=40_000_000_000, bytes_accessed=16_000_000, transcendentals=0),
    )(centered_t, grad_all, vh, means, weights, whiten.reshape(s.nz, s.fb, fb))

    return pl.pallas_call(
        final_kernel,
        name="final",
        grid=(s.nz,),
        out_shape=sd((tok, fb), BF16),
        in_specs=[
            pl.BlockSpec((tok, fb), lambda q: (0, 0)),
            pl.BlockSpec((1, tok, fb), lambda q: (q, 0, 0)),
            pl.BlockSpec((1, fb, fb), lambda q: (q, 0, 0)),
        ],
        out_specs=pl.BlockSpec((tok, fb), lambda q: (0, 0)),
        scratch_shapes=[pltpu.VMEM((tok, fb), F32)],
        compiler_params=pltpu.CompilerParams(dimension_semantics=("arbitrary",)),
        cost_estimate=pl.CostEstimate(flops=2 * tok * s.d * fb, bytes_accessed=6_000_000, transcendentals=0),
    )(acc, centered_all, sens)


def solution(mesh):
    in_specs = (P("rows", "feat"), P("rows", "feat"), P("feat", "rows"), P(), P(None, "feat"))
    out_specs = P("rows", "feat")
    return jax.shard_map(local, mesh=mesh, in_specs=in_specs, out_specs=out_specs, check_vma=False)
```

```python
import functools

import jax
import jax.numpy as jnp
from jax import lax
from jax.experimental import pallas as pl
from jax.experimental.pallas import tpu as pltpu
from jax.sharding import PartitionSpec as P

MESH = pl.DeviceIdType.MESH
F32 = jnp.float32
BF16 = jnp.bfloat16
VMEM_CAP = 62 * 1024 * 1024
CHUNKS = 4


class Dims:
    def __init__(self, rows, feat, tokens, d):
        self.nr, self.nz = rows, feat
        self.nk = rows // 2
        self.nx = {4: 2, 16: 4}[self.nk]
        self.ny = self.nk // self.nx
        self.kh = self.nk // 2
        self.d, self.dh = d, d // 2
        self.n = tokens
        self.tok = tokens // rows
        self.fb = d // feat
        self.fbh = self.fb // 2
        self.sr = self.fb // self.nk
        self.ea = d // self.nk
        self.er = d // rows
        self.hops = feat // 2
        self.chunk = self.tok // CHUNKS

    def slot(self, src, g):
        dist = (g - src) % self.nz
        if dist == 0:
            return 0
        if dist == self.hops:
            return self.nz - 1
        return 2 * dist if dist < self.hops else 2 * (self.nz - dist) - 1


def where_am_i():
    r = lax.axis_index("rows")
    z = lax.axis_index("feat")
    return r, z, r // 2, lax.rem(r, 2)


def send(src, dst, ss, rs, r, z):
    copy = pltpu.make_async_remote_copy(
        src, dst, ss, rs, device_id={"rows": r, "feat": z}, device_id_type=MESH
    )
    copy.start()


def arrive(ref, sem):
    pltpu.make_async_copy(ref, ref, sem).wait()


def greet(s, r, z):
    barrier = pltpu.get_barrier_semaphore()

    def plane(t, _):
        pl.semaphore_signal(
            barrier, 1, device_id={"rows": lax.rem(r + t, s.nr), "feat": z}, device_id_type=MESH
        )
        return 0

    def line(t, _):
        pl.semaphore_signal(
            barrier, 1, device_id={"rows": r, "feat": lax.rem(z + t, s.nz)}, device_id_type=MESH
        )
        return 0

    lax.fori_loop(1, s.nr, plane, 0)
    lax.fori_loop(1, s.nz, line, 0)
    pl.semaphore_wait(barrier, s.nr - 1 + s.nz - 1)


class Ring:
    def __init__(self, s, r, z, own, buf, ssem, hsem, rsem):
        self.s, self.r, self.z = s, r, z
        self.own, self.buf = own, buf
        self.ssem, self.hsem, self.rsem = ssem, hsem, rsem

    def block(self, way, h):
        nz = self.s.nz
        return lax.rem(self.z + (nz - h if way == 0 else h), nz)

    def rows(self, q):
        return pl.ds(q * self.s.chunk, self.s.chunk)

    def start(self, way, h, q):
        s = self.s
        to = lax.rem(self.z + (1 if way == 0 else s.nz - 1), s.nz)
        blk = self.block(way, h - 1)
        src = self.own.at[self.rows(q)] if h == 1 else self.buf.at[blk, self.rows(q)]
        ss = self.hsem if h == s.hops else self.ssem
        send(src, self.buf.at[blk, self.rows(q)], ss.at[way], self.rsem.at[way, h - 1, q], self.r, to)

    def has(self, way, h, q):
        return h < self.s.hops or (q < CHUNKS // 2) == (way == 0)

    def begin(self, qs):
        for q in qs:
            for way in (0, 1):
                self.start(way, 1, q)

    def step(self, h, qs):
        for q in qs:
            for way in (0, 1):
                if self.has(way, h, q):
                    arrive(self.buf.at[0, self.rows(q)], self.rsem.at[way, h - 1, q])
                    if h < self.s.hops and self.has(way, h + 1, q):
                        self.start(way, h + 1, q)

    def drain(self):
        s = self.s
        for way in (0, 1):
            arrive(self.buf.at[pl.ds(0, s.hops - 1)], self.ssem.at[way])
            arrive(self.buf.at[0, pl.ds(0, s.tok // 2)], self.hsem.at[way])


def whole_kernel(
    s, x_ref, g_ref, v_ref, e_ref, w_ref, out_ref,
    ga, xa, grid, vv, pad, pad_in, tile, m_out, m_in, mean, xct, acc, kk_buf,
    cp, cp_in, part, part_in, c128, t1s, t1r, mt, sy_out, sy_in, t2p, t2d, t2s, t2g,
    sp, sp_out, sp_in, sens,
    ssem, rsem, p2sem, lsem, gs, gh, gr, xs, xh, xr, ds_, dr_, rs_, rr_, zr_,
):
    r, z, k, c = where_am_i()
    y, x = k // s.nx, lax.rem(k, s.nx)
    mate = r + 1 - 2 * c
    first = c == 0
    a = jnp.where(first, x, y)
    b = jnp.where(first, y, x)
    half = k // s.kh
    mine = half == c
    kk = lax.rem(k, s.kh)
    every = range(CHUNKS)
    g_ring = Ring(s, r, z, g_ref, ga, gs, gh, gr)
    x_ring = Ring(s, r, z, xa.at[z], xa, xs, xh, xr)

    v = v_ref[...]
    twice = jnp.concatenate([v, v], axis=1)
    lane_half = lax.broadcasted_iota(jnp.int32, twice.shape, 1) // s.er
    pad[...] = jnp.where(lane_half == c, twice, 0.0).astype(BF16)
    sum_x = jnp.sum(x_ref[...].astype(F32), axis=0, keepdims=True)
    sum_g = jnp.sum(g_ref[...].astype(F32), axis=0, keepdims=True)
    m_out[0] = jnp.concatenate([sum_x, sum_g], axis=1)
    m_in[r] = m_out[0]

    greet(s, r, z)

    send(pad, pad_in, ssem.at[0], rsem.at[0], mate, z)
    g_ring.begin([0])

    def sums(t, _):
        send(m_out.at[0], m_in.at[r], ssem.at[1], rsem.at[1], lax.rem(r + t, s.nr), z)
        return 0

    lax.fori_loop(1, s.nr, sums, 0)
    arrive(pad_in, rsem.at[0])
    tile[...] = pad[...] + pad_in[...]
    grid[b, a, z] = tile[pl.ds(pl.multiple_of(c * s.fbh, s.fbh), s.fbh), :]

    def up(t, _):
        send(grid.at[b, a, z], grid.at[b, a, z], ssem.at[2], rsem.at[2], r, lax.rem(z + t, s.nz))
        return 0

    lax.fori_loop(1, s.nz, up, 0)
    g_ring.begin(every[1:])
    ga[z] = g_ref[...]

    arrive(m_in.at[pl.ds(0, s.nr - 1)], rsem.at[1])
    own_mean = jnp.sum(m_in[...], axis=0) / s.n
    mean[z] = own_mean

    def mean_up(t, _):
        send(mean.at[z], mean.at[z], ssem.at[3], rsem.at[3], r, lax.rem(z + t, s.nz))
        return 0

    lax.fori_loop(1, s.nz, mean_up, 0)
    centered = (x_ref[...].astype(F32) - own_mean[:, : s.fb]).astype(BF16)
    xa[z] = centered
    xct[...] = centered.astype(F32).T.astype(BF16)
    col_sum = jnp.sum(xct[...].astype(F32), axis=1, keepdims=True)
    acc[...] = jnp.zeros_like(acc)

    def gram(slot, blk):
        nu = mean[blk][:, s.fb :]
        prod = jnp.dot(xct[...], ga[blk], preferred_element_type=F32) - col_sum * nu
        cp[slot, 0] = prod[:, : s.fbh]
        cp[slot, 1] = prod[:, s.fbh :]

    def product(blk):
        nu = mean[blk][:, s.fb :]
        shifted = (ga[blk].astype(F32) - nu).astype(BF16)
        acc[...] += jnp.dot(shifted, w_ref[blk], preferred_element_type=F32)

    def round_of(h):
        if h == 0:
            return [(0, z)]
        if h == s.hops:
            return [(s.nz - 1, g_ring.block(0, h))]
        return [(2 * h - 1, g_ring.block(0, h)), (2 * h, g_ring.block(1, h))]

    def round_start(h):
        pairs = round_of(h)
        slots = pl.ds(pairs[0][0], len(pairs))
        for slot, blk in pairs:
            gram(slot, blk)
        send(cp.at[slots, 1 - c], cp_in.at[slots], ds_.at[h], dr_.at[h], mate, z)

    def round_scatter(h):
        pairs = round_of(h)
        slots = pl.ds(pairs[0][0], len(pairs))
        arrive(cp_in.at[slots], dr_.at[h])
        for slot, _ in pairs:
            both = cp[slot, c] + cp_in[slot]
            part[:, slot] = both.reshape(s.nk, s.sr, s.fbh).astype(BF16)

        def scatter(t, _):
            k2 = lax.rem(k + t, s.nk)
            send(part.at[k2, slots], part_in.at[k, slots], rs_.at[h], rr_.at[h], 2 * k2 + c, z)
            return 0

        lax.fori_loop(1, s.nk, scatter, 0)
        part_in[k, slots] = part[k, slots]

    def round_sum(hs, batch):
        for h in hs:
            arrive(part_in.at[pl.ds(0, s.nk - 1), pl.ds(0, len(round_of(h)))], rr_.at[h])
        lo = round_of(hs[0])[0][0]
        n = round_of(hs[-1])[-1][0] + 1 - lo
        slots = pl.ds(lo, n)
        c128[c, z, slots] = jnp.sum(part_in[:, slots].astype(F32), axis=0).astype(BF16)

        def lift(t, _):
            send(
                c128.at[c, z, slots], c128.at[c, z, slots], ssem.at[9 + batch], zr_.at[batch],
                r, lax.rem(z + t, s.nz),
            )
            return 0

        lax.fori_loop(1, s.nz, lift, 0)
        return slots

    arrive(mean.at[pl.ds(0, s.nz - 1)], rsem.at[3])
    round_start(0)

    arrive(grid.at[0, 0, pl.ds(0, s.nz - 1)], rsem.at[2])

    def along_a(t, _):
        a2 = lax.rem(a + t, s.nx)
        y2, x2 = jnp.where(first, y, a2), jnp.where(first, a2, x)
        send(grid.at[b, a], grid.at[b, a], ssem.at[4], rsem.at[4], (y2 * s.nx + x2) * 2 + c, z)
        return 0

    lax.fori_loop(1, s.nx, along_a, 0)
    round_scatter(0)
    product(z)

    def along_b(t, _):
        b2 = lax.rem(b + t, s.ny)
        y2, x2 = jnp.where(first, b2, y), jnp.where(first, x, b2)
        send(grid.at[b], grid.at[b], ssem.at[5], p2sem.at[t], (y2 * s.nx + x2) * 2 + c, z)
        return 0

    def hand_out(b2):
        def each(a2, _):
            y2, x2 = jnp.where(first, b2, a2), jnp.where(first, a2, b2)
            to = y2 // (s.ny // 2)
            pos = lax.rem(y2, s.ny // 2) * s.nx + x2
            cols = pl.ds(pl.multiple_of(pos * s.ea, s.ea), s.ea)
            dst = vv.at[:, c, :, cols]

            @pl.when(to == c)
            def _():
                pltpu.make_async_copy(grid.at[b2, a2], dst, lsem).start()

            @pl.when(to != c)
            def _():
                send(grid.at[b2, a2], dst, ssem.at[6], rsem.at[6], mate, z)

            return 0

        lax.fori_loop(0, s.nx, each, 0)

    arrive(grid.at[0, pl.ds(0, s.nx - 1)], rsem.at[4])
    lax.fori_loop(1, s.ny, along_b, 0)
    g_ring.step(1, every)
    hand_out(b)

    s_row = jnp.broadcast_to(lax.rsqrt(e_ref[k]), (s.ea, s.ea)).T
    for j in range(s.kh):
        s_col = lax.rsqrt(e_ref[c * s.kh + j])
        both = s_row * s_col
        kk_buf[:, j * s.ea : (j + 1) * s.ea] = -(both * both) / (s_row + s_col)

    for h in range(1, s.hops):
        round_start(h)
        round_scatter(h)
        for _, blk in round_of(h):
            product(blk)
        if h == s.hops - 1:
            round_sum(range(0, h), 0)
        g_ring.step(h + 1, every)

    round_start(s.hops)
    x_ring.begin(every[: CHUNKS // 2])
    round_scatter(s.hops)
    product(round_of(s.hops)[0][1])

    def landed(t, _):
        b2 = lax.rem(b + s.ny - t, s.ny)
        arrive(grid.at[b2], p2sem.at[t])
        hand_out(b2)
        return 0

    lax.fori_loop(1, s.ny, landed, 0)
    round_sum([s.hops - 1], 1)
    round_sum([s.hops], 2)
    x_ring.begin(every[CHUNKS // 2 :])

    early = round_of(s.hops - 2)[-1][0] + 1
    arrive(c128.at[c, pl.ds(0, s.nz - 1), pl.ds(0, early)], zr_.at[0])
    arrive(c128.at[c, pl.ds(0, s.nz - 1), pl.ds(0, s.nz - 1 - early)], zr_.at[1])
    arrive(c128.at[c, pl.ds(0, s.nz - 1), pl.ds(0, 1)], zr_.at[2])
    send(c128.at[c], c128.at[c], ssem.at[12], rsem.at[7], mate, z)
    arrive(vv.at[:, c], lsem)
    arrive(vv.at[:, 1 - c], rsem.at[6])

    def cross_rows(h):
        bands = []
        for src in range(s.nz):
            bands.append(jnp.concatenate([c128[h, src, s.slot(src, g)] for g in range(s.nz)], axis=1))
        return jnp.concatenate(bands, axis=0)

    def basis_rows(h):
        return vv[:, h].reshape(s.dh, s.dh)

    t1 = jnp.dot(cross_rows(c), basis_rows(c), preferred_element_type=F32)
    arrive(c128.at[1 - c], rsem.at[7])
    t1 += jnp.dot(cross_rows(1 - c), basis_rows(1 - c), preferred_element_type=F32)
    for j in range(s.kh):
        t1s[j] = t1[:, j * s.ea : (j + 1) * s.ea].astype(BF16).reshape(s.nz, s.sr, s.ea)

    def turn(t, _):
        j = lax.rem(kk + t, s.kh)
        k2 = c * s.kh + j

        @pl.when(k2 != k)
        def _():
            send(t1s.at[j], t1r.at[:, k], ssem.at[7], rsem.at[8], 2 * k2 + c, z)

        send(t1s.at[j], t1r.at[:, k], ssem.at[8], rsem.at[8], 2 * k2 + 1 - c, z)
        return 0

    lax.fori_loop(0, s.kh, turn, 0)
    x_ring.step(1, every)

    @pl.when(mine)
    def _():
        t1r[:, k] = t1s[kk]
        arrive(t1r.at[:, pl.ds(0, s.nk - 1)], rsem.at[8])
        arrive(t1s.at[pl.ds(0, s.kh - 1)], ssem.at[7])

    @pl.when(jnp.logical_not(mine))
    def _():
        arrive(t1r, rsem.at[8])
        arrive(t1s, ssem.at[7])

    left = t1r[...].reshape(s.d, s.ea).astype(F32).T.astype(BF16)
    mt[...] = jnp.dot(left, vv[...].reshape(s.d, s.dh), preferred_element_type=F32)
    for j in range(s.kh):
        sy_out[j] = mt[:, j * s.ea : (j + 1) * s.ea].T.astype(BF16)

    def mirror(t, _):
        j = lax.rem(kk + t, s.kh)
        k2 = c * s.kh + j

        @pl.when(k2 != k)
        def _():
            send(sy_out.at[j], sy_in.at[kk], ssem.at[13], rsem.at[9], 2 * k2 + half, z)

        return 0

    lax.fori_loop(0, s.kh, mirror, 0)
    x_ring.step(2, every[: CHUNKS // 2])

    @pl.when(mine)
    def _():
        sy_in[kk] = sy_out[kk]
        arrive(sy_in.at[pl.ds(0, s.kh - 1)], rsem.at[9])
        arrive(sy_out.at[pl.ds(0, s.kh - 1)], ssem.at[13])

    @pl.when(jnp.logical_not(mine))
    def _():
        arrive(sy_in, rsem.at[9])
        arrive(sy_out, ssem.at[13])

    total = jnp.zeros((s.ea, s.fb), F32)
    own_rows = vv.at[z]
    for j in range(s.kh):
        cols = slice(j * s.ea, (j + 1) * s.ea)
        rotated = 0.5 * (mt[:, cols] + sy_in[j].astype(F32))
        weighted = (kk_buf[:, cols] * rotated).astype(BF16)
        right = own_rows[:, :, cols].reshape(s.fb, s.ea)
        total += lax.dot_general(
            weighted, right, (((1,), (1,)), ((), ())), preferred_element_type=F32
        )
    t2p[...] = total
    send(t2p, t2d, ssem.at[14], rsem.at[10], mate, z)
    x_ring.step(2, every[CHUNKS // 2 :])
    arrive(t2d, rsem.at[10])
    t2s[...] = (t2p[...] + t2d[...]).astype(BF16).reshape(t2s.shape)

    def spread(t, _):
        k2 = lax.rem(k + t, s.nk)
        send(t2s.at[c], t2g.at[kk, c], ssem.at[15], rsem.at[11], 2 * k2 + half, z)
        return 0

    lax.fori_loop(1, s.nk, spread, 0)
    x_ring.step(3, every)

    @pl.when(mine)
    def _():
        t2g[kk] = t2s[...]
        arrive(t2g.at[pl.ds(0, s.kh - 1)], rsem.at[11])

    @pl.when(jnp.logical_not(mine))
    def _():
        arrive(t2g, rsem.at[11])

    right2 = t2g[...].reshape(s.dh, s.fb)

    def back(q, _):
        prod = jnp.dot(vv[q].reshape(s.fb, s.dh), right2, preferred_element_type=F32)
        prod = prod * (2.0 / s.n)
        sp[q] = prod
        sp_out[q] = prod.astype(BF16)
        send(sp_out.at[q], sp_in.at[q], ssem.at[16], rsem.at[12], mate, z)
        return 0

    lax.fori_loop(0, s.nz, back, 0)
    arrive(sp_in, rsem.at[12])
    for q in range(s.nz):
        sens[q] = (sp[q] + sp_in[q].astype(F32)).astype(BF16)

    x_ring.step(s.hops, every)

    def last(m, _):
        rows = pl.ds(pl.multiple_of(m * s.chunk, s.chunk), s.chunk)
        res = acc[rows, :]
        for q in range(s.nz):
            res += jnp.dot(xa[q, rows, :], sens[q], preferred_element_type=F32)
        out_ref[rows, :] = res.astype(BF16)
        return 0

    lax.fori_loop(0, CHUNKS, last, 0)

    g_ring.drain()
    x_ring.drain()
    arrive(pad, ssem.at[0])
    arrive(m_in.at[pl.ds(0, s.nr - 1)], ssem.at[1])
    arrive(grid.at[0, 0, pl.ds(0, s.nz - 1)], ssem.at[2])
    arrive(mean.at[pl.ds(0, s.nz - 1)], ssem.at[3])
    arrive(grid.at[0, pl.ds(0, s.nx - 1)], ssem.at[4])
    arrive(grid.at[pl.ds(0, s.ny - 1)], ssem.at[5])
    arrive(vv.at[:, c], ssem.at[6])
    arrive(t1s, ssem.at[8])
    arrive(c128.at[c, pl.ds(0, s.nz - 1), pl.ds(0, early)], ssem.at[9])
    arrive(c128.at[c, pl.ds(0, s.nz - 1), pl.ds(0, s.nz - 1 - early)], ssem.at[10])
    arrive(c128.at[c, pl.ds(0, s.nz - 1), pl.ds(0, 1)], ssem.at[11])
    arrive(c128.at[c], ssem.at[12])
    arrive(t2p, ssem.at[14])
    arrive(part.at[pl.ds(0, s.nk - 1)], ssem.at[15])
    arrive(sp_out, ssem.at[16])
    for h in range(s.hops + 1):
        n = len(round_of(h))
        arrive(cp_in.at[pl.ds(0, n)], ds_.at[h])
        arrive(part_in.at[pl.ds(0, s.nk - 1), pl.ds(0, n)], rs_.at[h])


def local(features, grad_out, eigvecs, eigvals, whiten):
    tok, fb = features.shape
    s = Dims(lax.axis_size("rows"), lax.axis_size("feat"), tok * lax.axis_size("rows"), whiten.shape[0])
    dma = pltpu.SemaphoreType.DMA
    vmem = pltpu.VMEM
    vm = pl.BlockSpec(memory_space=pltpu.VMEM)
    return pl.pallas_call(
        functools.partial(whole_kernel, s),
        name="whole",
        out_shape=jax.ShapeDtypeStruct((tok, fb), BF16),
        in_specs=[vm] * 5,
        out_specs=vm,
        scratch_shapes=[
            vmem((s.nz, tok, fb), BF16),
            vmem((s.nz, tok, fb), BF16),
            vmem((s.ny, s.nx, s.nz, s.fbh, s.ea), BF16),
            vmem((s.nz, 2, s.fbh, s.dh), BF16),
            vmem((s.fb, s.ea), BF16),
            vmem((s.fb, s.ea), BF16),
            vmem((s.fb, s.ea), BF16),
            vmem((1, 1, 2 * s.fb), F32),
            vmem((s.nr, 1, 2 * s.fb), F32),
            vmem((s.nz, 1, 2 * s.fb), F32),
            vmem((fb, tok), BF16),
            vmem((tok, fb), F32),
            vmem((s.ea, s.dh), F32),
            vmem((s.nz, 2, s.fb, s.fbh), F32),
            vmem((s.nz, s.fb, s.fbh), F32),
            vmem((s.nk, s.nz, s.sr, s.fbh), BF16),
            vmem((s.nk, s.nz, s.sr, s.fbh), BF16),
            vmem((2, s.nz, s.nz, s.sr, s.fbh), BF16),
            vmem((s.kh, s.nz, s.sr, s.ea), BF16),
            vmem((s.nz, s.nk, s.sr, s.ea), BF16),
            vmem((s.ea, s.dh), F32),
            vmem((s.kh, s.ea, s.ea), BF16),
            vmem((s.kh, s.ea, s.ea), BF16),
            vmem((s.ea, s.fb), F32),
            vmem((s.ea, s.fb), F32),
            vmem((2, s.ea // 2, s.fb), BF16),
            vmem((s.kh, 2, s.ea // 2, s.fb), BF16),
            vmem((s.nz, s.fb, s.fb), F32),
            vmem((s.nz, s.fb, s.fb), BF16),
            vmem((s.nz, s.fb, s.fb), BF16),
            vmem((s.nz, s.fb, s.fb), BF16),
            dma((17,)),
            dma((13,)),
            dma((s.ny,)),
            dma,
            dma((2,)),
            dma((2,)),
            dma((2, s.hops, CHUNKS)),
            dma((2,)),
            dma((2,)),
            dma((2, s.hops, CHUNKS)),
            dma((s.hops + 1,)),
            dma((s.hops + 1,)),
            dma((s.hops + 1,)),
            dma((s.hops + 1,)),
            dma((3,)),
        ],
        compiler_params=pltpu.CompilerParams(
            collective_id=0, has_side_effects=True, vmem_limit_bytes=VMEM_CAP
        ),
        cost_estimate=pl.CostEstimate(flops=60_000_000_000, bytes_accessed=16_000_000, transcendentals=0),
    )(features, grad_out, eigvecs, eigvals.reshape(s.nk, 1, s.ea), whiten.reshape(s.nz, s.fb, fb))


def solution(mesh):
    in_specs = (P("rows", "feat"), P("rows", "feat"), P("feat", "rows"), P(), P(None, "feat"))
    out_specs = P("rows", "feat")
    return jax.shard_map(local, mesh=mesh, in_specs=in_specs, out_specs=out_specs, check_vma=False)
```

```python
import functools

import jax
import jax.numpy as jnp
from jax import lax
from jax.experimental import pallas as pl
from jax.experimental.pallas import tpu as pltpu
from jax.sharding import PartitionSpec as P

MESH = pl.DeviceIdType.MESH
F32 = jnp.float32
BF16 = jnp.bfloat16
VMEM_CAP = 62 * 1024 * 1024
CHUNKS = 4


class Dims:
    def __init__(self, rows, feat, tokens, d):
        self.nr, self.nz = rows, feat
        self.nk = rows // 2
        self.nx = {4: 2, 16: 4}[self.nk]
        self.ny = self.nk // self.nx
        self.kh = self.nk // 2
        self.d, self.dh = d, d // 2
        self.n = tokens
        self.tok = tokens // rows
        self.fb = d // feat
        self.fbh = self.fb // 2
        self.sr = self.fb // self.nk
        self.ea = d // self.nk
        self.er = d // rows
        self.hops = feat // 2
        self.chunk = self.tok // CHUNKS

    def slot(self, src, g):
        dist = (g - src) % self.nz
        if dist == 0:
            return 0
        if dist == self.hops:
            return self.nz - 1
        return 2 * dist if dist < self.hops else 2 * (self.nz - dist) - 1


def where_am_i():
    r = lax.axis_index("rows")
    z = lax.axis_index("feat")
    return r, z, r // 2, lax.rem(r, 2)


def send(src, dst, ss, rs, r, z):
    copy = pltpu.make_async_remote_copy(
        src, dst, ss, rs, device_id={"rows": r, "feat": z}, device_id_type=MESH
    )
    copy.start()


def arrive(ref, sem):
    pltpu.make_async_copy(ref, ref, sem).wait()


def greet(s, r, z):
    barrier = pltpu.get_barrier_semaphore()

    def plane(t, _):
        pl.semaphore_signal(
            barrier, 1, device_id={"rows": lax.rem(r + t, s.nr), "feat": z}, device_id_type=MESH
        )
        return 0

    def line(t, _):
        pl.semaphore_signal(
            barrier, 1, device_id={"rows": r, "feat": lax.rem(z + t, s.nz)}, device_id_type=MESH
        )
        return 0

    lax.fori_loop(1, s.nr, plane, 0)
    lax.fori_loop(1, s.nz, line, 0)
    return lambda: pl.semaphore_wait(barrier, s.nr - 1 + s.nz - 1)


class Ring:
    def __init__(self, s, r, z, own, buf, ssem, hsem, rsem):
        self.s, self.r, self.z = s, r, z
        self.own, self.buf = own, buf
        self.ssem, self.hsem, self.rsem = ssem, hsem, rsem

    def block(self, way, h):
        nz = self.s.nz
        return lax.rem(self.z + (nz - h if way == 0 else h), nz)

    def rows(self, q):
        return pl.ds(q * self.s.chunk, self.s.chunk)

    def start(self, way, h, q):
        s = self.s
        to = lax.rem(self.z + (1 if way == 0 else s.nz - 1), s.nz)
        blk = self.block(way, h - 1)
        src = self.own.at[self.rows(q)] if h == 1 else self.buf.at[blk, self.rows(q)]
        ss = self.hsem if h == s.hops else self.ssem
        send(src, self.buf.at[blk, self.rows(q)], ss.at[way], self.rsem.at[way, h - 1, q], self.r, to)

    def has(self, way, h, q):
        return h < self.s.hops or (q < CHUNKS // 2) == (way == 0)

    def begin(self, qs):
        for q in qs:
            for way in (0, 1):
                self.start(way, 1, q)

    def step(self, h, qs):
        for q in qs:
            for way in (0, 1):
                if self.has(way, h, q):
                    arrive(self.buf.at[0, self.rows(q)], self.rsem.at[way, h - 1, q])
                    if h < self.s.hops and self.has(way, h + 1, q):
                        self.start(way, h + 1, q)

    def drain(self):
        s = self.s
        for way in (0, 1):
            arrive(self.buf.at[pl.ds(0, s.hops - 1)], self.ssem.at[way])
            arrive(self.buf.at[0, pl.ds(0, s.tok // 2)], self.hsem.at[way])


class Axis:
    def __init__(self, n, pos, device, z, block, part, ssem, rsem):
        self.n, self.pos, self.device, self.z = n, pos, device, z
        self.block, self.part, self.ssem, self.rsem = block, part, ssem, rsem
        self.right = lax.rem(pos + 1, n)
        self.left = lax.rem(pos + n - 1, n)
        self.far = lax.rem(pos + 2, n)

    def put(self, ref, sem, to):
        send(ref, ref, self.ssem, self.rsem.at[sem], self.device(to), self.z)

    def start(self):
        self.put(self.block(self.pos), 0, self.right)
        if self.n > 2:
            self.put(self.block(self.pos), 1, self.left)

    def forward(self):
        arrive(self.block(0), self.rsem.at[0])
        if self.n > 2:
            self.put(self.part(self.left, 0), 2, self.right)
            arrive(self.block(0), self.rsem.at[1])
            self.put(self.part(self.right, 1), 3, self.left)

    def finish(self):
        if self.n > 2:
            arrive(self.part(0, 0), self.rsem.at[2])
            arrive(self.part(0, 1), self.rsem.at[3])


def whole_kernel(
    s, x_hbm, g_hbm, v_ref, e_ref, w_hbm, out_ref,
    x_ref, g_ref, w_ref, ga, xa, grid, vv, pad, pad_in, tile, m_out, m_in, mean, xct, acc, kk_buf,
    cp, cp_in, part, part_in, c128, t1s, t1r, mt, sy_out, sy_in, t2p, t2d, t2s, t2g,
    sp, sp_out, sp_in, sens,
    ssem, rsem, asem, bsem, lsem, isem, gs, gh, gr, xs, xh, xr, ds_, dr_, rs_, rr_, zr_,
):
    r, z, k, c = where_am_i()
    y, x = k // s.nx, lax.rem(k, s.nx)
    mate = r + 1 - 2 * c
    first = c == 0
    a = jnp.where(first, x, y)
    b = jnp.where(first, y, x)
    half = k // s.kh
    mine = half == c
    kk = lax.rem(k, s.kh)
    every = range(CHUNKS)
    g_ring = Ring(s, r, z, g_ref, ga, gs, gh, gr)
    x_ring = Ring(s, r, z, xa.at[z], xa, xs, xh, xr)

    welcome = greet(s, r, z)
    loads = [
        pltpu.make_async_copy(src, dst, isem.at[i])
        for i, (src, dst) in enumerate(((g_hbm, g_ref), (x_hbm, x_ref), (w_hbm, w_ref)))
    ]
    for load in loads:
        load.start()
    v = v_ref[...].T
    twice = jnp.concatenate([v, v], axis=1)
    lane_half = lax.broadcasted_iota(jnp.int32, twice.shape, 1) // s.er
    pad[...] = jnp.where(lane_half == c, twice, 0.0).astype(BF16)
    loads[0].wait()
    loads[1].wait()
    sum_x = jnp.sum(x_ref[...].astype(F32), axis=0, keepdims=True)
    sum_g = jnp.sum(g_ref[...].astype(F32), axis=0, keepdims=True)
    m_out[0] = jnp.concatenate([sum_x, sum_g], axis=1)
    m_in[r] = m_out[0]

    welcome()

    send(pad, pad_in, ssem.at[0], rsem.at[0], mate, z)
    g_ring.begin([0])

    def sums(t, _):
        send(m_out.at[0], m_in.at[r], ssem.at[1], rsem.at[1], lax.rem(r + t, s.nr), z)
        return 0

    lax.fori_loop(1, s.nr, sums, 0)
    arrive(pad_in, rsem.at[0])
    tile[...] = pad[...] + pad_in[...]
    grid[b, a, z] = tile[pl.ds(pl.multiple_of(c * s.fbh, s.fbh), s.fbh), :]

    def up(t, _):
        send(grid.at[b, a, z], grid.at[b, a, z], ssem.at[2], rsem.at[2], r, lax.rem(z + t, s.nz))
        return 0

    lax.fori_loop(1, s.nz, up, 0)
    g_ring.begin([1])
    ga[z] = g_ref[...]

    s_row = jnp.broadcast_to(lax.rsqrt(e_ref[k]), (s.ea, s.ea)).T
    for j in range(s.kh):
        s_col = lax.rsqrt(e_ref[c * s.kh + j])
        both = s_row * s_col
        kk_buf[:, j * s.ea : (j + 1) * s.ea] = -(both * both) / (s_row + s_col)
    acc[...] = jnp.zeros_like(acc)
    loads[2].wait()

    arrive(m_in.at[pl.ds(0, s.nr - 1)], rsem.at[1])
    own_mean = jnp.sum(m_in[...], axis=0) / s.n
    mean[z] = own_mean

    def mean_up(t, _):
        send(mean.at[z], mean.at[z], ssem.at[3], rsem.at[3], r, lax.rem(z + t, s.nz))
        return 0

    lax.fori_loop(1, s.nz, mean_up, 0)
    g_ring.begin([2, 3])
    centered = (x_ref[...].astype(F32) - own_mean[:, : s.fb]).astype(BF16)
    xa[z] = centered
    xct[...] = centered.astype(F32).T.astype(BF16)
    col_sum = jnp.sum(xct[...].astype(F32), axis=1, keepdims=True)

    def gram(slot, blk):
        nu = mean[blk][:, s.fb :]
        prod = jnp.dot(xct[...], ga[blk], preferred_element_type=F32) - col_sum * nu
        cp[slot, 0] = prod[:, : s.fbh]
        cp[slot, 1] = prod[:, s.fbh :]

    def product(blk):
        nu = mean[blk][:, s.fb :]
        shifted = (ga[blk].astype(F32) - nu).astype(BF16)
        acc[...] += jnp.dot(shifted, w_ref[blk], preferred_element_type=F32)

    def round_of(h):
        if h == 0:
            return [(0, z)]
        if h == s.hops:
            return [(s.nz - 1, g_ring.block(0, h))]
        return [(2 * h - 1, g_ring.block(0, h)), (2 * h, g_ring.block(1, h))]

    def round_start(h):
        pairs = round_of(h)
        slots = pl.ds(pairs[0][0], len(pairs))
        for slot, blk in pairs:
            gram(slot, blk)
        send(cp.at[slots, 1 - c], cp_in.at[slots], ds_.at[h], dr_.at[h], mate, z)

    def round_scatter(h):
        pairs = round_of(h)
        slots = pl.ds(pairs[0][0], len(pairs))
        arrive(cp_in.at[slots], dr_.at[h])
        for slot, _ in pairs:
            both = cp[slot, c] + cp_in[slot]
            part[:, slot] = both.reshape(s.nk, s.sr, s.fbh).astype(BF16)

        def scatter(t, _):
            k2 = lax.rem(k + t, s.nk)
            send(part.at[k2, slots], part_in.at[k, slots], rs_.at[h], rr_.at[h], 2 * k2 + c, z)
            return 0

        lax.fori_loop(1, s.nk, scatter, 0)
        part_in[k, slots] = part[k, slots]

    def round_sum(hs, batch):
        for h in hs:
            arrive(part_in.at[pl.ds(0, s.nk - 1), pl.ds(0, len(round_of(h)))], rr_.at[h])
        lo = round_of(hs[0])[0][0]
        n = round_of(hs[-1])[-1][0] + 1 - lo
        slots = pl.ds(lo, n)
        c128[c, z, slots] = jnp.sum(part_in[:, slots].astype(F32), axis=0).astype(BF16)

        def lift(t, _):
            send(
                c128.at[c, z, slots], c128.at[c, z, slots], ssem.at[9 + batch], zr_.at[batch],
                r, lax.rem(z + t, s.nz),
            )
            return 0

        lax.fori_loop(1, s.nz, lift, 0)
        return slots

    assert s.nx == s.ny and s.nx in (2, 4)
    nzh, nxh = s.nz // 2, s.nx // 2

    def device(a2, b2):
        y2, x2 = jnp.where(first, b2, a2), jnp.where(first, a2, b2)
        return (y2 * s.nx + x2) * 2 + c

    axis_a = Axis(
        s.nx, a, lambda p: device(p, b), z, lambda p: grid.at[b, p],
        lambda p, i: grid.at[b, p, pl.ds(i * nzh, nzh)], ssem.at[4], asem,
    )
    axis_b = Axis(
        s.ny, b, lambda p: device(a, p), z, lambda p: grid.at[p],
        lambda p, i: grid.at[p, pl.ds(i * nxh, nxh)], ssem.at[5], bsem,
    )

    def hand_out(b2):
        def each(a2, _):
            y2, x2 = jnp.where(first, b2, a2), jnp.where(first, a2, b2)
            to = y2 // (s.ny // 2)
            pos = lax.rem(y2, s.ny // 2) * s.nx + x2
            cols = pl.ds(pl.multiple_of(pos * s.ea, s.ea), s.ea)
            dst = vv.at[:, c, :, cols]

            @pl.when(to == c)
            def _():
                pltpu.make_async_copy(grid.at[b2, a2], dst, lsem).start()

            @pl.when(to != c)
            def _():
                send(grid.at[b2, a2], dst, ssem.at[6], rsem.at[6], mate, z)

            return 0

        lax.fori_loop(0, s.nx, each, 0)

    arrive(grid.at[0, 0, pl.ds(0, s.nz - 1)], rsem.at[2])
    axis_a.start()
    g_ring.step(1, every[:2])
    arrive(mean.at[pl.ds(0, s.nz - 1)], rsem.at[3])
    axis_a.forward()
    round_start(0)
    g_ring.step(1, every[2:3])
    axis_a.finish()
    axis_b.start()
    round_scatter(0)
    g_ring.step(1, every[3:])
    hand_out(b)

    for h in range(1, s.hops):
        round_start(h)
        for _, blk in round_of(h - 1):
            product(blk)
        round_scatter(h)
        if h == s.hops - 2:
            axis_b.forward()
            hand_out(axis_b.left)
            if s.ny > 2:
                hand_out(axis_b.right)
        if h == s.hops - 1:
            g_ring.step(h + 1, every[:1])
            round_sum(range(0, h), 0)
            g_ring.step(h + 1, every[1:])
        else:
            g_ring.step(h + 1, every)

    round_start(s.hops)
    x_ring.begin([0])
    round_scatter(s.hops)
    round_sum([s.hops - 1], 1)
    for h in (s.hops - 1, s.hops):
        for _, blk in round_of(h):
            product(blk)

    round_sum([s.hops], 2)
    x_ring.begin(every[1:])
    axis_b.finish()
    if s.ny > 2:
        hand_out(axis_b.far)

    early = round_of(s.hops - 2)[-1][0] + 1
    arrive(c128.at[c, pl.ds(0, s.nz - 1), pl.ds(0, early)], zr_.at[0])
    arrive(c128.at[c, pl.ds(0, s.nz - 1), pl.ds(0, s.nz - 1 - early)], zr_.at[1])
    arrive(c128.at[c, pl.ds(0, s.nz - 1), pl.ds(0, 1)], zr_.at[2])
    send(c128.at[c], c128.at[c], ssem.at[12], rsem.at[7], mate, z)
    arrive(vv.at[:, c], lsem)
    arrive(vv.at[:, 1 - c], rsem.at[6])

    def cross_rows(h):
        bands = []
        for src in range(s.nz):
            bands.append(jnp.concatenate([c128[h, src, s.slot(src, g)] for g in range(s.nz)], axis=1))
        return jnp.concatenate(bands, axis=0)

    crosses = [cross_rows(c)]
    arrive(c128.at[1 - c], rsem.at[7])
    crosses.append(cross_rows(1 - c))
    for t in range(s.kh // 2):
        pair = lax.rem(kk // 2 + t, s.kh // 2)
        cols = pl.ds(pl.multiple_of(pair * 2 * s.ea, 2 * s.ea), 2 * s.ea)
        t1 = sum(
            jnp.dot(
                crosses[i], vv[:, h, :, cols].reshape(s.dh, 2 * s.ea), preferred_element_type=F32
            )
            for i, h in enumerate((c, 1 - c))
        )
        for i in range(2):
            j = pair * 2 + i
            k2 = c * s.kh + j
            t1s[j] = t1[:, i * s.ea : (i + 1) * s.ea].astype(BF16).reshape(s.nz, s.sr, s.ea)

            @pl.when(k2 != k)
            def _():
                send(t1s.at[j], t1r.at[:, k], ssem.at[7], rsem.at[8], 2 * k2 + c, z)

            send(t1s.at[j], t1r.at[:, k], ssem.at[8], rsem.at[8], 2 * k2 + 1 - c, z)

    x_ring.step(1, every)

    @pl.when(mine)
    def _():
        t1r[:, k] = t1s[kk]
        arrive(t1r.at[:, pl.ds(0, s.nk - 1)], rsem.at[8])
        arrive(t1s.at[pl.ds(0, s.kh - 1)], ssem.at[7])

    @pl.when(jnp.logical_not(mine))
    def _():
        arrive(t1r, rsem.at[8])
        arrive(t1s, ssem.at[7])

    left = t1r[...].reshape(s.d, s.ea).astype(F32).T.astype(BF16)
    mt[...] = jnp.dot(left, vv[...].reshape(s.d, s.dh), preferred_element_type=F32)
    for j in range(s.kh):
        sy_out[j] = mt[:, j * s.ea : (j + 1) * s.ea].T.astype(BF16)

    def mirror(t, _):
        j = lax.rem(kk + t, s.kh)
        k2 = c * s.kh + j

        @pl.when(k2 != k)
        def _():
            send(sy_out.at[j], sy_in.at[kk], ssem.at[13], rsem.at[9], 2 * k2 + half, z)

        return 0

    lax.fori_loop(0, s.kh, mirror, 0)
    x_ring.step(2, every[:2])

    @pl.when(mine)
    def _():
        sy_in[kk] = sy_out[kk]
        arrive(sy_in.at[pl.ds(0, s.kh - 1)], rsem.at[9])
        arrive(sy_out.at[pl.ds(0, s.kh - 1)], ssem.at[13])

    @pl.when(jnp.logical_not(mine))
    def _():
        arrive(sy_in, rsem.at[9])
        arrive(sy_out, ssem.at[13])

    total = jnp.zeros((s.ea, s.fb), F32)
    own_rows = vv.at[z]
    for j in range(s.kh):
        cols = slice(j * s.ea, (j + 1) * s.ea)
        rotated = 0.5 * (mt[:, cols] + sy_in[j].astype(F32))
        weighted = (kk_buf[:, cols] * rotated).astype(BF16)
        right = own_rows[:, :, cols].reshape(s.fb, s.ea)
        total += lax.dot_general(
            weighted, right, (((1,), (1,)), ((), ())), preferred_element_type=F32
        )
    t2p[...] = total
    send(t2p, t2d, ssem.at[14], rsem.at[10], mate, z)
    x_ring.step(2, every[2:])
    arrive(t2d, rsem.at[10])
    t2s[...] = (t2p[...] + t2d[...]).astype(BF16).reshape(t2s.shape)

    def spread(t, _):
        k2 = lax.rem(k + t, s.nk)
        send(t2s.at[c], t2g.at[kk, c], ssem.at[15], rsem.at[11], 2 * k2 + half, z)
        return 0

    lax.fori_loop(1, s.nk, spread, 0)
    x_ring.step(3, every)

    @pl.when(mine)
    def _():
        t2g[kk] = t2s[...]
        arrive(t2g.at[pl.ds(0, s.kh - 1)], rsem.at[11])

    @pl.when(jnp.logical_not(mine))
    def _():
        arrive(t2g, rsem.at[11])

    right2 = t2g[...].reshape(s.dh, s.fb)

    def back(q, _):
        prod = jnp.dot(vv[q].reshape(s.fb, s.dh), right2, preferred_element_type=F32)
        prod = prod * (2.0 / s.n)
        sp[q] = prod
        sp_out[q] = prod.astype(BF16)
        send(sp_out.at[q], sp_in.at[q], ssem.at[16], rsem.at[12], mate, z)
        return 0

    lax.fori_loop(0, s.nz, back, 0)
    arrive(sp_in, rsem.at[12])
    for q in range(s.nz):
        sens[q] = (sp[q] + sp_in[q].astype(F32)).astype(BF16)

    x_ring.step(s.hops, every)

    def last(m, _):
        rows = pl.ds(pl.multiple_of(m * s.chunk, s.chunk), s.chunk)
        res = acc[rows, :]
        for q in range(s.nz):
            res += jnp.dot(xa[q, rows, :], sens[q], preferred_element_type=F32)
        out_ref[rows, :] = res.astype(BF16)
        return 0

    lax.fori_loop(0, CHUNKS, last, 0)

    g_ring.drain()
    x_ring.drain()
    arrive(pad, ssem.at[0])
    arrive(m_in.at[pl.ds(0, s.nr - 1)], ssem.at[1])
    arrive(grid.at[0, 0, pl.ds(0, s.nz - 1)], ssem.at[2])
    arrive(mean.at[pl.ds(0, s.nz - 1)], ssem.at[3])
    arrive(grid.at[0, pl.ds(0, s.nx - 1)], ssem.at[4])
    arrive(grid.at[pl.ds(0, s.ny - 1)], ssem.at[5])
    arrive(vv.at[:, c], ssem.at[6])
    arrive(t1s, ssem.at[8])
    arrive(c128.at[c, pl.ds(0, s.nz - 1), pl.ds(0, early)], ssem.at[9])
    arrive(c128.at[c, pl.ds(0, s.nz - 1), pl.ds(0, s.nz - 1 - early)], ssem.at[10])
    arrive(c128.at[c, pl.ds(0, s.nz - 1), pl.ds(0, 1)], ssem.at[11])
    arrive(c128.at[c], ssem.at[12])
    arrive(t2p, ssem.at[14])
    arrive(part.at[pl.ds(0, s.nk - 1)], ssem.at[15])
    arrive(sp_out, ssem.at[16])
    for h in range(s.hops + 1):
        n = len(round_of(h))
        arrive(cp_in.at[pl.ds(0, n)], ds_.at[h])
        arrive(part_in.at[pl.ds(0, s.nk - 1), pl.ds(0, n)], rs_.at[h])


def local(features, grad_out, eigvecs, eigvals, whiten):
    tok, fb = features.shape
    s = Dims(lax.axis_size("rows"), lax.axis_size("feat"), tok * lax.axis_size("rows"), whiten.shape[0])
    dma = pltpu.SemaphoreType.DMA
    vmem = pltpu.VMEM
    vm = pl.BlockSpec(memory_space=pltpu.VMEM)
    hbm = pl.BlockSpec(memory_space=pl.ANY)
    return pl.pallas_call(
        functools.partial(whole_kernel, s),
        name="whole",
        out_shape=jax.ShapeDtypeStruct((tok, fb), BF16),
        in_specs=[hbm, hbm, vm, vm, hbm],
        out_specs=vm,
        scratch_shapes=[
            vmem((tok, fb), BF16),
            vmem((tok, fb), BF16),
            vmem((s.nz, s.fb, fb), BF16),
            vmem((s.nz, tok, fb), BF16),
            vmem((s.nz, tok, fb), BF16),
            vmem((s.ny, s.nx, s.nz, s.fbh, s.ea), BF16),
            vmem((s.nz, 2, s.fbh, s.dh), BF16),
            vmem((s.fb, s.ea), BF16),
            vmem((s.fb, s.ea), BF16),
            vmem((s.fb, s.ea), BF16),
            vmem((1, 1, 2 * s.fb), F32),
            vmem((s.nr, 1, 2 * s.fb), F32),
            vmem((s.nz, 1, 2 * s.fb), F32),
            vmem((fb, tok), BF16),
            vmem((tok, fb), F32),
            vmem((s.ea, s.dh), F32),
            vmem((s.nz, 2, s.fb, s.fbh), F32),
            vmem((s.nz, s.fb, s.fbh), F32),
            vmem((s.nk, s.nz, s.sr, s.fbh), BF16),
            vmem((s.nk, s.nz, s.sr, s.fbh), BF16),
            vmem((2, s.nz, s.nz, s.sr, s.fbh), BF16),
            vmem((s.kh, s.nz, s.sr, s.ea), BF16),
            vmem((s.nz, s.nk, s.sr, s.ea), BF16),
            vmem((s.ea, s.dh), F32),
            vmem((s.kh, s.ea, s.ea), BF16),
            vmem((s.kh, s.ea, s.ea), BF16),
            vmem((s.ea, s.fb), F32),
            vmem((s.ea, s.fb), F32),
            vmem((2, s.ea // 2, s.fb), BF16),
            vmem((s.kh, 2, s.ea // 2, s.fb), BF16),
            vmem((s.nz, s.fb, s.fb), F32),
            vmem((s.nz, s.fb, s.fb), BF16),
            vmem((s.nz, s.fb, s.fb), BF16),
            vmem((s.nz, s.fb, s.fb), BF16),
            dma((17,)),
            dma((13,)),
            dma((4,)),
            dma((4,)),
            dma,
            dma((3,)),
            dma((2,)),
            dma((2,)),
            dma((2, s.hops, CHUNKS)),
            dma((2,)),
            dma((2,)),
            dma((2, s.hops, CHUNKS)),
            dma((s.hops + 1,)),
            dma((s.hops + 1,)),
            dma((s.hops + 1,)),
            dma((s.hops + 1,)),
            dma((3,)),
        ],
        compiler_params=pltpu.CompilerParams(
            collective_id=0, has_side_effects=True, vmem_limit_bytes=VMEM_CAP
        ),
        cost_estimate=pl.CostEstimate(flops=60_000_000_000, bytes_accessed=16_000_000, transcendentals=0),
    )(features, grad_out, eigvecs.T, eigvals.reshape(s.nk, 1, s.ea), whiten.reshape(s.nz, s.fb, fb))


def solution(mesh):
    in_specs = (P("rows", "feat"), P("rows", "feat"), P("feat", "rows"), P(), P(None, "feat"))
    out_specs = P("rows", "feat")
    return jax.shard_map(local, mesh=mesh, in_specs=in_specs, out_specs=out_specs, check_vma=False)
```

```python
import functools

import jax
import jax.numpy as jnp
from jax import lax
from jax.experimental import pallas as pl
from jax.experimental.pallas import tpu as pltpu
from jax.sharding import PartitionSpec as P

MESH = pl.DeviceIdType.MESH
F32 = jnp.float32
BF16 = jnp.bfloat16
VMEM_CAP = 62 * 1024 * 1024
CHUNKS = 8
ROW_TILES = 2


class Dims:
    def __init__(self, rows, feat, tokens, d):
        self.nr, self.nz = rows, feat
        self.nk = rows // 2
        self.nx = {4: 2, 16: 4}[self.nk]
        self.ny = self.nk // self.nx
        self.kh = self.nk // 2
        self.d, self.dh = d, d // 2
        self.n = tokens
        self.tok = tokens // rows
        self.fb = d // feat
        self.fbh = self.fb // 2
        self.sr = self.fb // self.nk
        self.ea = d // self.nk
        self.er = d // rows
        self.hops = feat // 2

    def slot(self, src, g):
        dist = (g - src) % self.nz
        if dist == 0:
            return 0
        if dist == self.hops:
            return self.nz - 1
        return 2 * dist if dist < self.hops else 2 * (self.nz - dist) - 1


def where_am_i():
    r = lax.axis_index("rows")
    z = lax.axis_index("feat")
    return r, z, r // 2, lax.rem(r, 2)


def send(src, dst, ss, rs, r, z):
    copy = pltpu.make_async_remote_copy(
        src, dst, ss, rs, device_id={"rows": r, "feat": z}, device_id_type=MESH
    )
    copy.start()


def arrive(ref, sem):
    pltpu.make_async_copy(ref, ref, sem).wait()


def greet(s, r, z):
    barrier = pltpu.get_barrier_semaphore()

    def plane(t, _):
        pl.semaphore_signal(
            barrier, 1, device_id={"rows": lax.rem(r + t, s.nr), "feat": z}, device_id_type=MESH
        )
        return 0

    def line(t, _):
        pl.semaphore_signal(
            barrier, 1, device_id={"rows": r, "feat": lax.rem(z + t, s.nz)}, device_id_type=MESH
        )
        return 0

    lax.fori_loop(1, s.nr, plane, 0)
    lax.fori_loop(1, s.nz, line, 0)
    return lambda: pl.semaphore_wait(barrier, s.nr - 1 + s.nz - 1)


class Ring:
    def __init__(self, s, r, z, own, buf, chunks, ssem, hsem, rsem):
        self.s, self.r, self.z = s, r, z
        self.own, self.buf, self.chunks = own, buf, chunks
        self.size = buf.shape[1] // chunks
        self.ssem, self.hsem, self.rsem = ssem, hsem, rsem
        self.done = set()

    def new(self, h, qs):
        fresh = [q for q in qs if (h, q) not in self.done]
        self.done.update((h, q) for q in fresh)
        return fresh

    def block(self, way, h):
        nz = self.s.nz
        return lax.rem(self.z + (nz - h if way == 0 else h), nz)

    def rows(self, q):
        return pl.ds(q * self.size, self.size)

    def start(self, way, h, q):
        s = self.s
        to = lax.rem(self.z + (1 if way == 0 else s.nz - 1), s.nz)
        blk = self.block(way, h - 1)
        src = self.own.at[self.rows(q)] if h == 1 else self.buf.at[blk, self.rows(q)]
        ss = self.hsem if h == s.hops else self.ssem
        send(src, self.buf.at[blk, self.rows(q)], ss.at[way], self.rsem.at[h - 1, q], self.r, to)

    def has(self, way, h, q):
        return h < self.s.hops or (q < self.chunks // 2) == (way == 0)

    def begin(self, qs):
        for q in self.new(0, qs):
            for way in (0, 1):
                self.start(way, 1, q)

    def step(self, h, qs):
        for q in self.new(h, qs):
            ways = [way for way in (0, 1) if self.has(way, h, q)]
            arrive(self.buf.at[0, pl.ds(0, len(ways) * self.size)], self.rsem.at[h - 1, q])
            for way in ways:
                if h < self.s.hops and self.has(way, h + 1, q):
                    self.start(way, h + 1, q)

    def drain(self):
        for way in (0, 1):
            arrive(self.buf.at[pl.ds(0, self.s.hops - 1)], self.ssem.at[way])
            arrive(self.buf.at[0, pl.ds(0, self.buf.shape[1] // 2)], self.hsem.at[way])


class Axis:
    def __init__(self, n, pos, device, z, block, part, ssem, rsem):
        self.n, self.pos, self.device, self.z = n, pos, device, z
        self.block, self.part, self.ssem, self.rsem = block, part, ssem, rsem
        self.right = lax.rem(pos + 1, n)
        self.left = lax.rem(pos + n - 1, n)
        self.far = lax.rem(pos + 2, n)

    def put(self, ref, sem, to):
        send(ref, ref, self.ssem, self.rsem.at[sem], self.device(to), self.z)

    def start(self):
        self.put(self.block(self.pos), 0, self.right)
        if self.n > 2:
            self.put(self.block(self.pos), 1, self.left)

    def forward(self):
        arrive(self.block(0), self.rsem.at[0])
        if self.n > 2:
            self.put(self.part(self.left, 0), 2, self.right)
            arrive(self.block(0), self.rsem.at[1])
            self.put(self.part(self.right, 1), 3, self.left)

    def finish(self):
        if self.n > 2:
            arrive(self.part(0, 0), self.rsem.at[2])
            arrive(self.part(0, 1), self.rsem.at[3])


def whole_kernel(
    s, x_hbm, g_hbm, v_hbm, e_hbm, w_hbm, out_ref,
    x_ref, g_ref, v_ref, e_ref, w_ref, ga, xa, grid, vv, pad, pad_in, tile, m_out, m_in, mean, xct, acc, kk_buf,
    cp, cp_in, part, part_in, c128, t1s, t1r, mt, sy_out, sy_in, t2p, t2d, t2s, t2g,
    sp, sp_out, sp_in, sens,
    ssem, rsem, asem, bsem, bfar, lsem, isem, gs, gh, gr, xs, xh, xr, vs, vh, vr, ds_, dr_, rs_, rr_, zr_,
):
    r, z, k, c = where_am_i()
    y, x = k // s.nx, lax.rem(k, s.nx)
    mate = r + 1 - 2 * c
    first = c == 0
    a = jnp.where(first, x, y)
    b = jnp.where(first, y, x)
    half = k // s.kh
    mine = half == c
    kk = lax.rem(k, s.kh)
    every = range(CHUNKS)
    g_ring = Ring(s, r, z, g_ref, ga, CHUNKS, gs, gh, gr)
    x_ring = Ring(s, r, z, xa.at[z], xa, CHUNKS, xs, xh, xr)
    v_ring = Ring(s, r, z, grid.at[b, a, z], grid.at[b, a], 2, vs, vh, vr)

    welcome = greet(s, r, z)
    inputs = (v_hbm, v_ref), (g_hbm, g_ref), (x_hbm, x_ref), (e_hbm, e_ref), (w_hbm, w_ref)
    loads = [
        pltpu.make_async_copy(src, dst, isem.at[i])
        for i, (src, dst) in enumerate(inputs)
    ]
    for load in loads:
        load.start()
    loads[0].wait()
    v = v_ref[...].T
    twice = jnp.concatenate([v, v], axis=1)
    lane_half = lax.broadcasted_iota(jnp.int32, twice.shape, 1) // s.er
    pad[...] = jnp.where(lane_half == c, twice, 0.0).astype(BF16)
    loads[1].wait()
    loads[2].wait()
    sum_x = jnp.sum(x_ref[...].astype(F32), axis=0, keepdims=True)
    sum_g = jnp.sum(g_ref[...].astype(F32), axis=0, keepdims=True)
    m_out[0] = jnp.concatenate([sum_x, sum_g], axis=1)
    m_in[r] = m_out[0]

    welcome()

    send(pad, pad_in, ssem.at[0], rsem.at[0], mate, z)
    g_ring.begin([0])

    def sums(t, _):
        send(m_out.at[0], m_in.at[r], ssem.at[1], rsem.at[1], lax.rem(r + t, s.nr), z)
        return 0

    lax.fori_loop(1, s.nr, sums, 0)
    arrive(pad_in, rsem.at[0])
    tile[...] = pad[...] + pad_in[...]
    grid[b, a, z] = tile[pl.ds(pl.multiple_of(c * s.fbh, s.fbh), s.fbh), :]

    v_ring.begin([0, 1])
    g_ring.begin([1, 2, 3])
    ga[z] = g_ref[...]

    loads[3].wait()
    s_row = jnp.broadcast_to(lax.rsqrt(e_ref[k]), (s.ea, s.ea)).T
    for j in range(s.kh):
        s_col = lax.rsqrt(e_ref[c * s.kh + j])
        both = s_row * s_col
        kk_buf[:, j * s.ea : (j + 1) * s.ea] = -(both * both) / (s_row + s_col)
    acc[...] = jnp.zeros_like(acc)
    loads[4].wait()
    v_ring.step(1, [0, 1])
    g_ring.begin([4, 5])

    arrive(m_in.at[pl.ds(0, s.nr - 1)], rsem.at[1])
    own_mean = jnp.sum(m_in[...], axis=0) / s.n
    mean[z] = own_mean

    def mean_up(t, _):
        send(mean.at[z], mean.at[z], ssem.at[3], rsem.at[3], r, lax.rem(z + t, s.nz))
        return 0

    lax.fori_loop(1, s.nz, mean_up, 0)
    if s.hops > 2:
        v_ring.step(2, [0, 1])
    g_ring.begin([6, 7])
    centered = (x_ref[...].astype(F32) - own_mean[:, : s.fb]).astype(BF16)
    xa[z] = centered
    xct[...] = centered.astype(F32).T.astype(BF16)
    col_sum = jnp.sum(xct[...].astype(F32), axis=1, keepdims=True)

    def gram(slot, blk):
        nu = mean[blk][:, s.fb :]
        prod = jnp.dot(xct[...], ga[blk], preferred_element_type=F32) - col_sum * nu
        cp[slot, 0] = prod[:, : s.fbh]
        cp[slot, 1] = prod[:, s.fbh :]

    def product(blk):
        nu = mean[blk][:, s.fb :]
        shifted = (ga[blk].astype(F32) - nu).astype(BF16)
        acc[...] += jnp.dot(shifted, w_ref[blk], preferred_element_type=F32)

    def round_of(h):
        if h == 0:
            return [(0, z)]
        if h == s.hops:
            return [(s.nz - 1, g_ring.block(0, h))]
        return [(2 * h - 1, g_ring.block(0, h)), (2 * h, g_ring.block(1, h))]

    def round_start(h):
        pairs = round_of(h)
        slots = pl.ds(pairs[0][0], len(pairs))
        for slot, blk in pairs:
            gram(slot, blk)
        send(cp.at[slots, 1 - c], cp_in.at[slots], ds_.at[h], dr_.at[h], mate, z)

    def round_scatter(h):
        pairs = round_of(h)
        slots = pl.ds(pairs[0][0], len(pairs))
        arrive(cp_in.at[slots], dr_.at[h])
        for slot, _ in pairs:
            both = cp[slot, c] + cp_in[slot]
            part[:, slot] = both.reshape(s.nk, s.sr, s.fbh).astype(BF16)

        def scatter(t, _):
            k2 = lax.rem(k + t, s.nk)
            send(part.at[k2, slots], part_in.at[k, slots], rs_.at[h], rr_.at[h], 2 * k2 + c, z)
            return 0

        lax.fori_loop(1, s.nk, scatter, 0)
        part_in[k, slots] = part[k, slots]

    def round_sum(hs, batch):
        for h in hs:
            arrive(part_in.at[pl.ds(0, s.nk - 1), pl.ds(0, len(round_of(h)))], rr_.at[h])
        lo = round_of(hs[0])[0][0]
        n = round_of(hs[-1])[-1][0] + 1 - lo
        slots = pl.ds(lo, n)
        c128[c, z, slots] = jnp.sum(part_in[:, slots].astype(F32), axis=0).astype(BF16)

        def lift(t, _):
            send(
                c128.at[c, z, slots], c128.at[c, z, slots], ssem.at[9 + batch], zr_.at[batch],
                r, lax.rem(z + t, s.nz),
            )
            return 0

        lax.fori_loop(1, s.nz, lift, 0)
        return slots

    assert s.nx == s.ny and s.nx in (2, 4)
    nzh = s.nz // 2

    def device(a2, b2):
        y2, x2 = jnp.where(first, b2, a2), jnp.where(first, a2, b2)
        return (y2 * s.nx + x2) * 2 + c

    axis_a = Axis(
        s.nx, a, lambda p: device(p, b), z, lambda p: grid.at[b, p],
        lambda p, i: grid.at[b, p, pl.ds(i * nzh, nzh)], ssem.at[4], asem,
    )
    b_right, b_left = lax.rem(b + 1, s.ny), lax.rem(b + s.ny - 1, s.ny)
    b_far = lax.rem(b + 2, s.ny)
    pieces = [a, axis_a.left] + ([axis_a.right, axis_a.far] if s.nx > 2 else [])

    def put_b(b2, piece, sem, to):
        ref = grid.at[b2, pieces[piece]]
        send(ref, ref, ssem.at[5], sem, device(a, to), z)

    def b_start(piece):
        put_b(b, piece, bsem.at[0, piece], b_right)
        if s.ny > 2:
            put_b(b, piece, bsem.at[1, piece], b_left)

    def b_forward():
        for piece in range(len(pieces)):
            arrive(grid.at[0, 0], bsem.at[0, piece])
            if s.ny > 2:
                if piece % 2 == 0:
                    put_b(b_left, piece, bfar.at[piece], b_right)
                arrive(grid.at[0, 0], bsem.at[1, piece])
                if piece % 2 == 1:
                    put_b(b_right, piece, bfar.at[piece], b_left)

    def b_finish():
        if s.ny > 2:
            for piece in range(len(pieces)):
                arrive(grid.at[0, 0], bfar.at[piece])

    def hand_out(b2):
        def each(a2, _):
            y2, x2 = jnp.where(first, b2, a2), jnp.where(first, a2, b2)
            to = y2 // (s.ny // 2)
            pos = lax.rem(y2, s.ny // 2) * s.nx + x2
            cols = pl.ds(pl.multiple_of(pos * s.ea, s.ea), s.ea)
            dst = vv.at[:, c, :, cols]

            @pl.when(to == c)
            def _():
                pltpu.make_async_copy(grid.at[b2, a2], dst, lsem).start()

            @pl.when(to != c)
            def _():
                send(grid.at[b2, a2], dst, ssem.at[6], rsem.at[6], mate, z)

            return 0

        lax.fori_loop(0, s.nx, each, 0)

    if s.hops > 3:
        v_ring.step(3, [0, 1])
    g_ring.step(1, every[:4])
    v_ring.step(s.hops, [0, 1])
    axis_a.start()
    b_start(0)
    g_ring.step(1, every[4:])
    arrive(mean.at[pl.ds(0, s.nz - 1)], rsem.at[3])
    round_start(0)
    g_ring.step(2, every[:3])
    axis_a.forward()
    b_start(1)
    if s.nx > 2:
        b_start(2)
    round_scatter(0)

    for h in range(1, s.hops):
        round_start(h)
        if h < s.hops - 1:
            g_ring.step(h + 1, every[:4])
        if h == 1:
            axis_a.finish()
            if s.nx > 2:
                b_start(3)
            hand_out(b)
        for _, blk in round_of(h - 1):
            product(blk)
        round_scatter(h)
        if h == s.hops - 1:
            b_forward()
            hand_out(b_left)
            if s.ny > 2:
                hand_out(b_right)
        g_ring.step(h + 1, every)
        if h == s.hops - 2:
            x_ring.begin(every[:4])

    round_start(s.hops)
    round_scatter(s.hops)
    round_sum(range(0, s.hops - 1), 0)
    round_sum([s.hops - 1], 1)
    for h in (s.hops - 1, s.hops):
        for _, blk in round_of(h):
            product(blk)

    round_sum([s.hops], 2)
    x_ring.begin(every)
    b_finish()
    if s.ny > 2:
        hand_out(b_far)

    early = round_of(s.hops - 2)[-1][0] + 1
    arrive(c128.at[c, pl.ds(0, s.nz - 1), pl.ds(0, early)], zr_.at[0])
    arrive(c128.at[c, pl.ds(0, s.nz - 1), pl.ds(0, s.nz - 1 - early)], zr_.at[1])
    arrive(c128.at[c, pl.ds(0, s.nz - 1), pl.ds(0, 1)], zr_.at[2])
    send(c128.at[c], c128.at[c], ssem.at[12], rsem.at[7], mate, z)
    arrive(vv.at[:, c], lsem)
    arrive(vv.at[:, 1 - c], rsem.at[6])

    def cross_rows(h):
        bands = []
        for src in range(s.nz):
            bands.append(jnp.concatenate([c128[h, src, s.slot(src, g)] for g in range(s.nz)], axis=1))
        return jnp.concatenate(bands, axis=0)

    mt[...] = jnp.dot(
        cross_rows(c), vv[:, c].reshape(s.dh, s.dh), preferred_element_type=F32
    )
    arrive(c128.at[1 - c], rsem.at[7])
    other = cross_rows(1 - c)
    for t in range(s.kh // 2):
        pair = lax.rem(kk // 2 + t, s.kh // 2)
        cols = pl.ds(pl.multiple_of(pair * 2 * s.ea, 2 * s.ea), 2 * s.ea)
        t1 = mt[:, cols] + jnp.dot(
            other, vv[:, 1 - c, :, cols].reshape(s.dh, 2 * s.ea), preferred_element_type=F32
        )
        for i in range(2):
            j = pair * 2 + i
            k2 = c * s.kh + j
            t1s[j] = t1[:, i * s.ea : (i + 1) * s.ea].astype(BF16).reshape(s.nz, s.sr, s.ea)

            @pl.when(k2 != k)
            def _():
                send(t1s.at[j], t1r.at[:, k], ssem.at[7], rsem.at[8], 2 * k2 + c, z)

            send(t1s.at[j], t1r.at[:, k], ssem.at[8], rsem.at[8], 2 * k2 + 1 - c, z)

    x_ring.step(1, every)

    @pl.when(mine)
    def _():
        t1r[:, k] = t1s[kk]
        arrive(t1r.at[:, pl.ds(0, s.nk - 1)], rsem.at[8])
        arrive(t1s.at[pl.ds(0, s.kh - 1)], ssem.at[7])

    @pl.when(jnp.logical_not(mine))
    def _():
        arrive(t1r, rsem.at[8])
        arrive(t1s, ssem.at[7])

    left = t1r[...].reshape(s.d, s.ea).astype(F32).T.astype(BF16)
    mt[...] = jnp.dot(left, vv[...].reshape(s.d, s.dh), preferred_element_type=F32)
    for j in range(s.kh):
        sy_out[j] = mt[:, j * s.ea : (j + 1) * s.ea].T.astype(BF16)

    def mirror(t, _):
        j = lax.rem(kk + t, s.kh)
        k2 = c * s.kh + j

        @pl.when(k2 != k)
        def _():
            send(sy_out.at[j], sy_in.at[kk], ssem.at[13], rsem.at[9], 2 * k2 + half, z)

        return 0

    lax.fori_loop(0, s.kh, mirror, 0)
    x_ring.step(2, every[:4])

    @pl.when(mine)
    def _():
        sy_in[kk] = sy_out[kk]
        arrive(sy_in.at[pl.ds(0, s.kh - 1)], rsem.at[9])
        arrive(sy_out.at[pl.ds(0, s.kh - 1)], ssem.at[13])

    @pl.when(jnp.logical_not(mine))
    def _():
        arrive(sy_in, rsem.at[9])
        arrive(sy_out, ssem.at[13])

    total = jnp.zeros((s.ea, s.fb), F32)
    own_rows = vv.at[z]
    for j in range(s.kh):
        cols = slice(j * s.ea, (j + 1) * s.ea)
        rotated = 0.5 * (mt[:, cols] + sy_in[j].astype(F32))
        weighted = (kk_buf[:, cols] * rotated).astype(BF16)
        right = own_rows[:, :, cols].reshape(s.fb, s.ea)
        total += lax.dot_general(
            weighted, right, (((1,), (1,)), ((), ())), preferred_element_type=F32
        )
    t2p[...] = total
    send(t2p, t2d, ssem.at[14], rsem.at[10], mate, z)
    x_ring.step(2, every[4:])
    arrive(t2d, rsem.at[10])
    t2s[...] = (t2p[...] + t2d[...]).astype(BF16).reshape(t2s.shape)

    def spread(t, _):
        k2 = lax.rem(k + t, s.nk)
        send(t2s.at[c], t2g.at[kk, c], ssem.at[15], rsem.at[11], 2 * k2 + half, z)
        return 0

    lax.fori_loop(1, s.nk, spread, 0)
    x_ring.step(3, every[:6])

    @pl.when(mine)
    def _():
        t2g[kk] = t2s[...]
        arrive(t2g.at[pl.ds(0, s.kh - 1)], rsem.at[11])

    @pl.when(jnp.logical_not(mine))
    def _():
        arrive(t2g, rsem.at[11])

    right2 = t2g[...].reshape(s.dh, s.fb)

    def back(q, _):
        two = pl.ds(2 * q, 2)
        left2 = vv[two].reshape(2 * s.fb, s.dh)
        prod = jnp.dot(left2, right2, preferred_element_type=F32) * (2.0 / s.n)
        prod = prod.reshape(2, s.fb, s.fb)
        sp[two] = prod
        sp_out[two] = prod.astype(BF16)
        send(sp_out.at[two], sp_in.at[two], ssem.at[16], rsem.at[12], mate, z)
        return 0

    lax.fori_loop(0, s.nz // 4, back, 0)
    x_ring.step(3, every[6:])
    lax.fori_loop(s.nz // 4, s.nz // 2, back, 0)
    arrive(sp_in, rsem.at[12])
    for q in range(s.nz):
        sens[q] = (sp[q] + sp_in[q].astype(F32)).astype(BF16)

    far = x_ring.block(0, s.hops)
    tile_rows = x_ref.shape[0] // ROW_TILES

    def most(m, _):
        rows = pl.ds(pl.multiple_of(m * tile_rows, tile_rows), tile_rows)
        res = acc[rows, :]
        for q in range(s.nz):
            if q != s.hops:
                blk = lax.rem(z + q, s.nz)
                res += jnp.dot(xa[blk, rows, :], sens[blk], preferred_element_type=F32)
        acc[rows, :] = res
        return 0

    lax.fori_loop(0, ROW_TILES, most, 0)
    x_ring.step(s.hops, every)

    def last(m, _):
        rows = pl.ds(pl.multiple_of(m * tile_rows, tile_rows), tile_rows)
        res = acc[rows, :] + jnp.dot(xa[far, rows, :], sens[far], preferred_element_type=F32)
        out_ref[rows, :] = res.astype(BF16)
        return 0

    lax.fori_loop(0, ROW_TILES, last, 0)

    g_ring.drain()
    x_ring.drain()
    arrive(pad, ssem.at[0])
    arrive(m_in.at[pl.ds(0, s.nr - 1)], ssem.at[1])
    v_ring.drain()
    arrive(mean.at[pl.ds(0, s.nz - 1)], ssem.at[3])
    arrive(grid.at[0, pl.ds(0, s.nx - 1)], ssem.at[4])
    arrive(grid.at[pl.ds(0, s.ny - 1)], ssem.at[5])
    arrive(vv.at[:, c], ssem.at[6])
    arrive(t1s, ssem.at[8])
    arrive(c128.at[c, pl.ds(0, s.nz - 1), pl.ds(0, early)], ssem.at[9])
    arrive(c128.at[c, pl.ds(0, s.nz - 1), pl.ds(0, s.nz - 1 - early)], ssem.at[10])
    arrive(c128.at[c, pl.ds(0, s.nz - 1), pl.ds(0, 1)], ssem.at[11])
    arrive(c128.at[c], ssem.at[12])
    arrive(t2p, ssem.at[14])
    arrive(part.at[pl.ds(0, s.nk - 1)], ssem.at[15])
    arrive(sp_out, ssem.at[16])
    for h in range(s.hops + 1):
        n = len(round_of(h))
        arrive(cp_in.at[pl.ds(0, n)], ds_.at[h])
        arrive(part_in.at[pl.ds(0, s.nk - 1), pl.ds(0, n)], rs_.at[h])


def local(features, grad_out, eigvecs, eigvals, whiten):
    tok, fb = features.shape
    s = Dims(lax.axis_size("rows"), lax.axis_size("feat"), tok * lax.axis_size("rows"), whiten.shape[0])
    dma = pltpu.SemaphoreType.DMA
    vmem = pltpu.VMEM
    vm = pl.BlockSpec(memory_space=pltpu.VMEM)
    hbm = pl.BlockSpec(memory_space=pl.ANY)
    return pl.pallas_call(
        functools.partial(whole_kernel, s),
        name="whole",
        out_shape=pltpu.VMEM((tok, fb), BF16),
        in_specs=[hbm] * 5,
        out_specs=vm,
        scratch_shapes=[
            vmem((tok, fb), BF16),
            vmem((tok, fb), BF16),
            vmem((s.er, s.fb), F32),
            vmem((s.nk, 1, s.ea), F32),
            vmem((s.nz, s.fb, fb), BF16),
            vmem((s.nz, tok, fb), BF16),
            vmem((s.nz, tok, fb), BF16),
            vmem((s.ny, s.nx, s.nz, s.fbh, s.ea), BF16),
            vmem((s.nz, 2, s.fbh, s.dh), BF16),
            vmem((s.fb, s.ea), BF16),
            vmem((s.fb, s.ea), BF16),
            vmem((s.fb, s.ea), BF16),
            vmem((1, 1, 2 * s.fb), F32),
            vmem((s.nr, 1, 2 * s.fb), F32),
            vmem((s.nz, 1, 2 * s.fb), F32),
            vmem((fb, tok), BF16),
            vmem((tok, fb), F32),
            vmem((s.ea, s.dh), F32),
            vmem((s.nz, 2, s.fb, s.fbh), F32),
            vmem((s.nz, s.fb, s.fbh), F32),
            vmem((s.nk, s.nz, s.sr, s.fbh), BF16),
            vmem((s.nk, s.nz, s.sr, s.fbh), BF16),
            vmem((2, s.nz, s.nz, s.sr, s.fbh), BF16),
            vmem((s.kh, s.nz, s.sr, s.ea), BF16),
            vmem((s.nz, s.nk, s.sr, s.ea), BF16),
            vmem((s.ea, s.dh), F32),
            vmem((s.kh, s.ea, s.ea), BF16),
            vmem((s.kh, s.ea, s.ea), BF16),
            vmem((s.ea, s.fb), F32),
            vmem((s.ea, s.fb), F32),
            vmem((2, s.ea // 2, s.fb), BF16),
            vmem((s.kh, 2, s.ea // 2, s.fb), BF16),
            vmem((s.nz, s.fb, s.fb), F32),
            vmem((s.nz, s.fb, s.fb), BF16),
            vmem((s.nz, s.fb, s.fb), BF16),
            vmem((s.nz, s.fb, s.fb), BF16),
            dma((17,)),
            dma((13,)),
            dma((4,)),
            dma((2, 4)),
            dma((4,)),
            dma,
            dma((5,)),
            dma((2,)),
            dma((2,)),
            dma((s.hops, CHUNKS)),
            dma((2,)),
            dma((2,)),
            dma((s.hops, CHUNKS)),
            dma((2,)),
            dma((2,)),
            dma((s.hops, 2)),
            dma((s.hops + 1,)),
            dma((s.hops + 1,)),
            dma((s.hops + 1,)),
            dma((s.hops + 1,)),
            dma((3,)),
        ],
        compiler_params=pltpu.CompilerParams(
            collective_id=0, has_side_effects=True, vmem_limit_bytes=VMEM_CAP
        ),
        cost_estimate=pl.CostEstimate(flops=60_000_000_000, bytes_accessed=16_000_000, transcendentals=0),
    )(features, grad_out, eigvecs.T, eigvals.reshape(s.nk, 1, s.ea), whiten.reshape(s.nz, s.fb, fb))


def solution(mesh):
    in_specs = (P("rows", "feat"), P("rows", "feat"), P("feat", "rows"), P(), P(None, "feat"))
    out_specs = P("rows", "feat")
    return jax.shard_map(local, mesh=mesh, in_specs=in_specs, out_specs=out_specs, check_vma=False)
```

```python
import functools

import jax
import jax.numpy as jnp
from jax import lax
from jax.experimental import pallas as pl
from jax.experimental.pallas import tpu as pltpu
from jax.sharding import PartitionSpec as P

MESH = pl.DeviceIdType.MESH
F32 = jnp.float32
BF16 = jnp.bfloat16
VMEM_CAP = 62 * 1024 * 1024
CHUNKS = 8
ROW_TILES = 2


class Dims:
    def __init__(self, rows, feat, tokens, d):
        self.nr, self.nz = rows, feat
        self.nk = rows // 2
        self.nx = {4: 2, 16: 4}[self.nk]
        self.ny = self.nk // self.nx
        self.kh = self.nk // 2
        self.d, self.dh = d, d // 2
        self.n = tokens
        self.tok = tokens // rows
        self.fb = d // feat
        self.fbh = self.fb // 2
        self.sr = self.fb // self.nk
        self.ea = d // self.nk
        self.er = d // rows
        self.hops = feat // 2

    def slot(self, src, g):
        dist = (g - src) % self.nz
        if dist == 0:
            return 0
        if dist == self.hops:
            return self.nz - 1
        return 2 * dist if dist < self.hops else 2 * (self.nz - dist) - 1


def where_am_i():
    r = lax.axis_index("rows")
    z = lax.axis_index("feat")
    return r, z, r // 2, lax.rem(r, 2)


def send(src, dst, ss, rs, r, z):
    copy = pltpu.make_async_remote_copy(
        src, dst, ss, rs, device_id={"rows": r, "feat": z}, device_id_type=MESH
    )
    copy.start()


def arrive(ref, sem):
    pltpu.make_async_copy(ref, ref, sem).wait()


def greet(s, r, z):
    barrier = pltpu.get_barrier_semaphore()

    def plane(t, _):
        pl.semaphore_signal(
            barrier, 1, device_id={"rows": lax.rem(r + t, s.nr), "feat": z}, device_id_type=MESH
        )
        return 0

    def line(t, _):
        pl.semaphore_signal(
            barrier, 1, device_id={"rows": r, "feat": lax.rem(z + t, s.nz)}, device_id_type=MESH
        )
        return 0

    lax.fori_loop(1, s.nr, plane, 0)
    lax.fori_loop(1, s.nz, line, 0)
    return lambda: pl.semaphore_wait(barrier, s.nr - 1 + s.nz - 1)


class Ring:
    def __init__(self, s, r, z, own, buf, cuts, ssem, hsem, rsem):
        self.s, self.r, self.z = s, r, z
        self.own, self.buf, self.cuts = own, buf, cuts
        self.ssem, self.hsem, self.rsem = ssem, hsem, rsem
        self.done = set()

    def new(self, h, qs):
        fresh = [q for q in qs if (h, q) not in self.done]
        self.done.update((h, q) for q in fresh)
        return fresh

    def block(self, way, h):
        nz = self.s.nz
        return lax.rem(self.z + (nz - h if way == 0 else h), nz)

    def rows(self, q):
        return pl.ds(*self.cuts[q])

    def start(self, way, h, q):
        s = self.s
        to = lax.rem(self.z + (1 if way == 0 else s.nz - 1), s.nz)
        blk = self.block(way, h - 1)
        src = self.own.at[self.rows(q)] if h == 1 else self.buf.at[blk, self.rows(q)]
        ss = self.hsem if h == s.hops else self.ssem
        send(src, self.buf.at[blk, self.rows(q)], ss.at[way], self.rsem.at[h - 1, q], self.r, to)

    def has(self, way, h, q):
        return h < self.s.hops or (q < len(self.cuts) // 2) == (way == 0)

    def begin(self, qs):
        for q in self.new(0, qs):
            for way in (0, 1):
                self.start(way, 1, q)

    def step(self, h, qs):
        for q in self.new(h, qs):
            ways = [way for way in (0, 1) if self.has(way, h, q)]
            both = pl.ds(0, len(ways) * self.cuts[q][1])
            arrive(self.buf.at[0, both], self.rsem.at[h - 1, q])
            for way in ways:
                if h < self.s.hops and self.has(way, h + 1, q):
                    self.start(way, h + 1, q)

    def drain(self):
        sizes = [size for _, size in self.cuts]
        half = len(sizes) // 2
        for way, far in ((0, sum(sizes[:half])), (1, sum(sizes[half:]))):
            near = self.buf.at[pl.ds(0, self.s.hops - 1), pl.ds(0, sum(sizes))]
            arrive(near, self.ssem.at[way])
            arrive(self.buf.at[0, pl.ds(0, far)], self.hsem.at[way])


def even(length, parts):
    return [(i * length // parts, length // parts) for i in range(parts)]


class Axis:
    def __init__(self, n, pos, device, z, block, part, ssem, rsem):
        self.n, self.pos, self.device, self.z = n, pos, device, z
        self.block, self.part, self.ssem, self.rsem = block, part, ssem, rsem
        self.right = lax.rem(pos + 1, n)
        self.left = lax.rem(pos + n - 1, n)
        self.far = lax.rem(pos + 2, n)

    def put(self, ref, sem, to):
        send(ref, ref, self.ssem, self.rsem.at[sem], self.device(to), self.z)

    def start(self):
        self.put(self.block(self.pos), 0, self.right)
        if self.n > 2:
            self.put(self.block(self.pos), 1, self.left)

    def forward(self):
        arrive(self.block(0), self.rsem.at[0])
        if self.n > 2:
            self.put(self.part(self.left, 0), 2, self.right)
            arrive(self.block(0), self.rsem.at[1])
            self.put(self.part(self.right, 1), 3, self.left)

    def finish(self):
        if self.n > 2:
            arrive(self.part(0, 0), self.rsem.at[2])
            arrive(self.part(0, 1), self.rsem.at[3])


def whole_kernel(
    s, x_hbm, g_hbm, v_hbm, e_hbm, w_hbm, out_ref,
    x_ref, g_ref, v_ref, e_ref, w_ref, ga, xa, grid, vv, pad, pad_in, tile, m_out, m_in, mean, xct, acc, kk_buf,
    cp, cp_in, part, part_in, c128, t1s, t1r, mt, sy_out, sy_in, t2p, t2d, t2s, t2g,
    sp, sp_out, sp_in, sens,
    ssem, rsem, asem, bsem, bfar, lsem, isem, gs, gh, gr, xs, xh, xr, vs, vh, vr, cs, ch, cr, ds_, dr_, rs_, rr_, zr_,
):
    r, z, k, c = where_am_i()
    y, x = k // s.nx, lax.rem(k, s.nx)
    mate = r + 1 - 2 * c
    first = c == 0
    a = jnp.where(first, x, y)
    b = jnp.where(first, y, x)
    half = k // s.kh
    mine = half == c
    kk = lax.rem(k, s.kh)
    every = range(CHUNKS)
    cuts = even(x_ref.shape[0], CHUNKS)
    early = 2 * s.hops - 3
    g_ring = Ring(s, r, z, g_ref, ga, cuts, gs, gh, gr)
    x_ring = Ring(s, r, z, xa.at[z], xa, cuts, xs, xh, xr)
    v_ring = Ring(s, r, z, grid.at[b, a, z], grid.at[b, a], even(s.fbh, 2), vs, vh, vr)
    early_cuts = [(0, (early + 1) // 2), ((early + 1) // 2, early // 2)]
    c_ring = Ring(s, r, z, c128.at[c, z], c128.at[c], early_cuts, cs, ch, cr)

    welcome = greet(s, r, z)
    inputs = (v_hbm, v_ref), (g_hbm, g_ref), (x_hbm, x_ref), (e_hbm, e_ref), (w_hbm, w_ref)
    loads = [
        pltpu.make_async_copy(src, dst, isem.at[i])
        for i, (src, dst) in enumerate(inputs)
    ]
    for load in loads:
        load.start()
    loads[0].wait()
    v = v_ref[...].T
    twice = jnp.concatenate([v, v], axis=1)
    lane_half = lax.broadcasted_iota(jnp.int32, twice.shape, 1) // s.er
    pad[...] = jnp.where(lane_half == c, twice, 0.0).astype(BF16)
    loads[1].wait()
    loads[2].wait()
    sum_x = jnp.sum(x_ref[...].astype(F32), axis=0, keepdims=True)
    sum_g = jnp.sum(g_ref[...].astype(F32), axis=0, keepdims=True)
    m_out[0] = jnp.concatenate([sum_x, sum_g], axis=1)
    m_in[r] = m_out[0]

    welcome()

    send(pad, pad_in, ssem.at[0], rsem.at[0], mate, z)
    g_ring.begin([0])

    def sums(t, _):
        send(m_out.at[0], m_in.at[r], ssem.at[1], rsem.at[1], lax.rem(r + t, s.nr), z)
        return 0

    lax.fori_loop(1, s.nr, sums, 0)
    arrive(pad_in, rsem.at[0])
    tile[...] = pad[...] + pad_in[...]
    grid[b, a, z] = tile[pl.ds(pl.multiple_of(c * s.fbh, s.fbh), s.fbh), :]

    v_ring.begin([0, 1])
    g_ring.begin([1, 2, 3])
    ga[z] = g_ref[...]

    loads[3].wait()
    s_row = jnp.broadcast_to(lax.rsqrt(e_ref[k]), (s.ea, s.ea)).T
    for j in range(s.kh):
        s_col = lax.rsqrt(e_ref[c * s.kh + j])
        both = s_row * s_col
        kk_buf[:, j * s.ea : (j + 1) * s.ea] = -(both * both) / (s_row + s_col)
    acc[...] = jnp.zeros_like(acc)
    loads[4].wait()
    v_ring.step(1, [0, 1])
    g_ring.begin([4, 5])

    arrive(m_in.at[pl.ds(0, s.nr - 1)], rsem.at[1])
    own_mean = jnp.sum(m_in[...], axis=0) / s.n
    mean[z] = own_mean

    def mean_up(t, _):
        send(mean.at[z], mean.at[z], ssem.at[3], rsem.at[3], r, lax.rem(z + t, s.nz))
        return 0

    lax.fori_loop(1, s.nz, mean_up, 0)
    if s.hops > 2:
        v_ring.step(2, [0, 1])
    g_ring.begin([6, 7])
    centered = (x_ref[...].astype(F32) - own_mean[:, : s.fb]).astype(BF16)
    xa[z] = centered
    xct[...] = centered.astype(F32).T.astype(BF16)
    col_sum = jnp.sum(xct[...].astype(F32), axis=1, keepdims=True)

    def gram(slot, blk):
        nu = mean[blk][:, s.fb :]
        prod = jnp.dot(xct[...], ga[blk], preferred_element_type=F32) - col_sum * nu
        cp[slot, 0] = prod[:, : s.fbh]
        cp[slot, 1] = prod[:, s.fbh :]

    def product(blk):
        nu = mean[blk][:, s.fb :]
        shifted = (ga[blk].astype(F32) - nu).astype(BF16)
        acc[...] += jnp.dot(shifted, w_ref[blk], preferred_element_type=F32)

    def round_of(h):
        if h == 0:
            return [(0, z)]
        if h == s.hops:
            return [(s.nz - 1, g_ring.block(0, h))]
        return [(2 * h - 1, g_ring.block(0, h)), (2 * h, g_ring.block(1, h))]

    def round_start(h):
        pairs = round_of(h)
        slots = pl.ds(pairs[0][0], len(pairs))
        for slot, blk in pairs:
            gram(slot, blk)
        send(cp.at[slots, 1 - c], cp_in.at[slots], ds_.at[h], dr_.at[h], mate, z)

    def round_scatter(h):
        pairs = round_of(h)
        slots = pl.ds(pairs[0][0], len(pairs))
        arrive(cp_in.at[slots], dr_.at[h])
        for slot, _ in pairs:
            both = cp[slot, c] + cp_in[slot]
            part[:, slot] = both.reshape(s.nk, s.sr, s.fbh).astype(BF16)

        def scatter(t, _):
            k2 = lax.rem(k + t, s.nk)
            send(part.at[k2, slots], part_in.at[k, slots], rs_.at[h], rr_.at[h], 2 * k2 + c, z)
            return 0

        lax.fori_loop(1, s.nk, scatter, 0)
        part_in[k, slots] = part[k, slots]

    def round_sum(hs):
        for h in hs:
            arrive(part_in.at[pl.ds(0, s.nk - 1), pl.ds(0, len(round_of(h)))], rr_.at[h])
        lo = round_of(hs[0])[0][0]
        n = round_of(hs[-1])[-1][0] + 1 - lo
        slots = pl.ds(lo, n)
        c128[c, z, slots] = jnp.sum(part_in[:, slots].astype(F32), axis=0).astype(BF16)

        return slots

    def round_lift(h, batch):
        slots = round_sum([h])

        def lift(t, _):
            send(
                c128.at[c, z, slots], c128.at[c, z, slots], ssem.at[9 + batch], zr_.at[batch],
                r, lax.rem(z + t, s.nz),
            )
            return 0

        lax.fori_loop(1, s.nz, lift, 0)

    assert s.nx == s.ny and s.nx in (2, 4)
    nzh = s.nz // 2

    def device(a2, b2):
        y2, x2 = jnp.where(first, b2, a2), jnp.where(first, a2, b2)
        return (y2 * s.nx + x2) * 2 + c

    axis_a = Axis(
        s.nx, a, lambda p: device(p, b), z, lambda p: grid.at[b, p],
        lambda p, i: grid.at[b, p, pl.ds(i * nzh, nzh)], ssem.at[4], asem,
    )
    b_right, b_left = lax.rem(b + 1, s.ny), lax.rem(b + s.ny - 1, s.ny)
    b_far = lax.rem(b + 2, s.ny)
    pieces = [a, axis_a.left] + ([axis_a.right, axis_a.far] if s.nx > 2 else [])

    def put_b(b2, piece, sem, to):
        ref = grid.at[b2, pieces[piece]]
        send(ref, ref, ssem.at[5], sem, device(a, to), z)

    def b_start(piece):
        put_b(b, piece, bsem.at[0, piece], b_right)
        if s.ny > 2:
            put_b(b, piece, bsem.at[1, piece], b_left)

    def b_forward():
        for piece in range(len(pieces)):
            arrive(grid.at[0, 0], bsem.at[0, piece])
            if s.ny > 2:
                if piece % 2 == 0:
                    put_b(b_left, piece, bfar.at[piece], b_right)
                arrive(grid.at[0, 0], bsem.at[1, piece])
                if piece % 2 == 1:
                    put_b(b_right, piece, bfar.at[piece], b_left)

    def b_finish():
        if s.ny > 2:
            for piece in range(len(pieces)):
                arrive(grid.at[0, 0], bfar.at[piece])

    def hand_out(b2):
        def each(a2, _):
            y2, x2 = jnp.where(first, b2, a2), jnp.where(first, a2, b2)
            to = y2 // (s.ny // 2)
            pos = lax.rem(y2, s.ny // 2) * s.nx + x2
            cols = pl.ds(pl.multiple_of(pos * s.ea, s.ea), s.ea)
            dst = vv.at[:, c, :, cols]

            @pl.when(to == c)
            def _():
                pltpu.make_async_copy(grid.at[b2, a2], dst, lsem).start()

            @pl.when(to != c)
            def _():
                send(grid.at[b2, a2], dst, ssem.at[6], rsem.at[6], mate, z)

            return 0

        lax.fori_loop(0, s.nx, each, 0)

    if s.hops > 3:
        v_ring.step(3, [0, 1])
    g_ring.step(1, every[:4])
    v_ring.step(s.hops, [0, 1])
    axis_a.start()
    b_start(0)
    g_ring.step(1, every[4:])
    arrive(mean.at[pl.ds(0, s.nz - 1)], rsem.at[3])
    round_start(0)
    g_ring.step(2, every[:3])
    axis_a.forward()
    b_start(1)
    if s.nx > 2:
        b_start(2)
    round_scatter(0)

    for h in range(1, s.hops):
        round_start(h)
        if h < s.hops - 1:
            g_ring.step(h + 1, every[:4])
        if h == 1:
            axis_a.finish()
            if s.nx > 2:
                b_start(3)
            hand_out(b)
        for _, blk in round_of(h - 1):
            product(blk)
        round_scatter(h)
        if h == s.hops - 1:
            round_sum(range(0, h))
            c_ring.begin([0, 1])
            x_ring.begin(every[:2])
            b_forward()
            hand_out(b_left)
            if s.ny > 2:
                hand_out(b_right)
        g_ring.step(h + 1, every)

    round_start(s.hops)
    if s.hops > 2:
        c_ring.step(1, [0, 1])
    x_ring.begin([2])
    round_scatter(s.hops)
    round_lift(s.hops - 1, 0)
    if s.hops > 2:
        c_ring.step(2, [0, 1])
    x_ring.begin([3, 4])
    for h in (s.hops - 1, s.hops):
        for _, blk in round_of(h):
            product(blk)
    round_lift(s.hops, 1)
    if s.hops > 2:
        c_ring.step(3, [0, 1])
    x_ring.begin(every)
    b_finish()
    if s.ny > 2:
        hand_out(b_far)

    c_ring.step(s.hops, [0, 1])
    arrive(c128.at[c, pl.ds(0, s.nz - 1), pl.ds(0, 2)], zr_.at[0])
    arrive(c128.at[c, pl.ds(0, s.nz - 1), pl.ds(0, 1)], zr_.at[1])
    send(c128.at[c], c128.at[c], ssem.at[12], rsem.at[7], mate, z)
    arrive(vv.at[:, c], lsem)
    arrive(vv.at[:, 1 - c], rsem.at[6])

    def cross_rows(h):
        bands = []
        for src in range(s.nz):
            bands.append(jnp.concatenate([c128[h, src, s.slot(src, g)] for g in range(s.nz)], axis=1))
        return jnp.concatenate(bands, axis=0)

    mt[...] = jnp.dot(
        cross_rows(c), vv[:, c].reshape(s.dh, s.dh), preferred_element_type=F32
    )
    arrive(c128.at[1 - c], rsem.at[7])
    other = cross_rows(1 - c)
    for t in range(s.kh // 2):
        pair = lax.rem(kk // 2 + t, s.kh // 2)
        cols = pl.ds(pl.multiple_of(pair * 2 * s.ea, 2 * s.ea), 2 * s.ea)
        t1 = mt[:, cols] + jnp.dot(
            other, vv[:, 1 - c, :, cols].reshape(s.dh, 2 * s.ea), preferred_element_type=F32
        )
        for i in range(2):
            j = pair * 2 + i
            k2 = c * s.kh + j
            t1s[j] = t1[:, i * s.ea : (i + 1) * s.ea].astype(BF16).reshape(s.nz, s.sr, s.ea)

            @pl.when(k2 != k)
            def _():
                send(t1s.at[j], t1r.at[:, k], ssem.at[7], rsem.at[8], 2 * k2 + c, z)

            send(t1s.at[j], t1r.at[:, k], ssem.at[8], rsem.at[8], 2 * k2 + 1 - c, z)

    x_ring.step(1, every)

    @pl.when(mine)
    def _():
        t1r[:, k] = t1s[kk]
        arrive(t1r.at[:, pl.ds(0, s.nk - 1)], rsem.at[8])
        arrive(t1s.at[pl.ds(0, s.kh - 1)], ssem.at[7])

    @pl.when(jnp.logical_not(mine))
    def _():
        arrive(t1r, rsem.at[8])
        arrive(t1s, ssem.at[7])

    left = t1r[...].reshape(s.d, s.ea).astype(F32).T.astype(BF16)
    mt[...] = jnp.dot(left, vv[...].reshape(s.d, s.dh), preferred_element_type=F32)
    for j in range(s.kh):
        sy_out[j] = mt[:, j * s.ea : (j + 1) * s.ea].T.astype(BF16)

    def mirror(t, _):
        j = lax.rem(kk + t, s.kh)
        k2 = c * s.kh + j

        @pl.when(k2 != k)
        def _():
            send(sy_out.at[j], sy_in.at[kk], ssem.at[13], rsem.at[9], 2 * k2 + half, z)

        return 0

    lax.fori_loop(0, s.kh, mirror, 0)
    x_ring.step(2, every[:4])

    @pl.when(mine)
    def _():
        sy_in[kk] = sy_out[kk]
        arrive(sy_in.at[pl.ds(0, s.kh - 1)], rsem.at[9])
        arrive(sy_out.at[pl.ds(0, s.kh - 1)], ssem.at[13])

    @pl.when(jnp.logical_not(mine))
    def _():
        arrive(sy_in, rsem.at[9])
        arrive(sy_out, ssem.at[13])

    total = jnp.zeros((s.ea, s.fb), F32)
    own_rows = vv.at[z]
    for j in range(s.kh):
        cols = slice(j * s.ea, (j + 1) * s.ea)
        rotated = 0.5 * (mt[:, cols] + sy_in[j].astype(F32))
        weighted = (kk_buf[:, cols] * rotated).astype(BF16)
        right = own_rows[:, :, cols].reshape(s.fb, s.ea)
        total += lax.dot_general(
            weighted, right, (((1,), (1,)), ((), ())), preferred_element_type=F32
        )
    t2p[...] = total
    send(t2p, t2d, ssem.at[14], rsem.at[10], mate, z)
    x_ring.step(2, every[4:])
    arrive(t2d, rsem.at[10])
    t2s[...] = (t2p[...] + t2d[...]).astype(BF16).reshape(t2s.shape)

    def spread(t, _):
        k2 = lax.rem(k + t, s.nk)
        send(t2s.at[c], t2g.at[kk, c], ssem.at[15], rsem.at[11], 2 * k2 + half, z)
        return 0

    lax.fori_loop(1, s.nk, spread, 0)
    x_ring.step(3, every[:6])

    @pl.when(mine)
    def _():
        t2g[kk] = t2s[...]
        arrive(t2g.at[pl.ds(0, s.kh - 1)], rsem.at[11])

    @pl.when(jnp.logical_not(mine))
    def _():
        arrive(t2g, rsem.at[11])

    right2 = t2g[...].reshape(s.dh, s.fb)

    def back(q, _):
        two = pl.ds(2 * q, 2)
        left2 = vv[two].reshape(2 * s.fb, s.dh)
        prod = jnp.dot(left2, right2, preferred_element_type=F32) * (2.0 / s.n)
        prod = prod.reshape(2, s.fb, s.fb)
        sp[two] = prod
        sp_out[two] = prod.astype(BF16)
        send(sp_out.at[two], sp_in.at[two], ssem.at[16], bsem.at[0, q], mate, z)
        return 0

    lax.fori_loop(0, s.nz // 4, back, 0)
    x_ring.step(3, every[6:])
    lax.fori_loop(s.nz // 4, s.nz // 2, back, 0)
    for q in range(s.nz):
        if q % 2 == 0:
            arrive(sp_in.at[pl.ds(0, 2)], bsem.at[0, q // 2])
        sens[q] = (sp[q] + sp_in[q].astype(F32)).astype(BF16)

    far = x_ring.block(0, s.hops)
    tile_rows = x_ref.shape[0] // ROW_TILES

    def most(m, _):
        rows = pl.ds(pl.multiple_of(m * tile_rows, tile_rows), tile_rows)
        res = acc[rows, :]
        for q in range(s.nz):
            if q != s.hops:
                blk = lax.rem(z + q, s.nz)
                res += jnp.dot(xa[blk, rows, :], sens[blk], preferred_element_type=F32)
        acc[rows, :] = res
        return 0

    lax.fori_loop(0, ROW_TILES, most, 0)
    x_ring.step(s.hops, every)

    def last(m, _):
        rows = pl.ds(pl.multiple_of(m * tile_rows, tile_rows), tile_rows)
        res = acc[rows, :] + jnp.dot(xa[far, rows, :], sens[far], preferred_element_type=F32)
        out_ref[rows, :] = res.astype(BF16)
        return 0

    lax.fori_loop(0, ROW_TILES, last, 0)

    g_ring.drain()
    x_ring.drain()
    arrive(pad, ssem.at[0])
    arrive(m_in.at[pl.ds(0, s.nr - 1)], ssem.at[1])
    v_ring.drain()
    arrive(mean.at[pl.ds(0, s.nz - 1)], ssem.at[3])
    arrive(grid.at[0, pl.ds(0, s.nx - 1)], ssem.at[4])
    arrive(grid.at[pl.ds(0, s.ny - 1)], ssem.at[5])
    arrive(vv.at[:, c], ssem.at[6])
    arrive(t1s, ssem.at[8])
    c_ring.drain()
    arrive(c128.at[c, pl.ds(0, s.nz - 1), pl.ds(0, 2)], ssem.at[9])
    arrive(c128.at[c, pl.ds(0, s.nz - 1), pl.ds(0, 1)], ssem.at[10])
    arrive(c128.at[c], ssem.at[12])
    arrive(t2p, ssem.at[14])
    arrive(part.at[pl.ds(0, s.nk - 1)], ssem.at[15])
    arrive(sp_out, ssem.at[16])
    for h in range(s.hops + 1):
        n = len(round_of(h))
        arrive(cp_in.at[pl.ds(0, n)], ds_.at[h])
        arrive(part_in.at[pl.ds(0, s.nk - 1), pl.ds(0, n)], rs_.at[h])


def local(features, grad_out, eigvecs, eigvals, whiten):
    tok, fb = features.shape
    s = Dims(lax.axis_size("rows"), lax.axis_size("feat"), tok * lax.axis_size("rows"), whiten.shape[0])
    dma = pltpu.SemaphoreType.DMA
    vmem = pltpu.VMEM
    vm = pl.BlockSpec(memory_space=pltpu.VMEM)
    hbm = pl.BlockSpec(memory_space=pl.ANY)
    return pl.pallas_call(
        functools.partial(whole_kernel, s),
        name="whole",
        out_shape=pltpu.VMEM((tok, fb), BF16),
        in_specs=[hbm] * 5,
        out_specs=vm,
        scratch_shapes=[
            vmem((tok, fb), BF16),
            vmem((tok, fb), BF16),
            vmem((s.er, s.fb), F32),
            vmem((s.nk, 1, s.ea), F32),
            vmem((s.nz, s.fb, fb), BF16),
            vmem((s.nz, tok, fb), BF16),
            vmem((s.nz, tok, fb), BF16),
            vmem((s.ny, s.nx, s.nz, s.fbh, s.ea), BF16),
            vmem((s.nz, 2, s.fbh, s.dh), BF16),
            vmem((s.fb, s.ea), BF16),
            vmem((s.fb, s.ea), BF16),
            vmem((s.fb, s.ea), BF16),
            vmem((1, 1, 2 * s.fb), F32),
            vmem((s.nr, 1, 2 * s.fb), F32),
            vmem((s.nz, 1, 2 * s.fb), F32),
            vmem((fb, tok), BF16),
            vmem((tok, fb), F32),
            vmem((s.ea, s.dh), F32),
            vmem((s.nz, 2, s.fb, s.fbh), F32),
            vmem((s.nz, s.fb, s.fbh), F32),
            vmem((s.nk, s.nz, s.sr, s.fbh), BF16),
            vmem((s.nk, s.nz, s.sr, s.fbh), BF16),
            vmem((2, s.nz, s.nz, s.sr, s.fbh), BF16),
            vmem((s.kh, s.nz, s.sr, s.ea), BF16),
            vmem((s.nz, s.nk, s.sr, s.ea), BF16),
            vmem((s.ea, s.dh), F32),
            vmem((s.kh, s.ea, s.ea), BF16),
            vmem((s.kh, s.ea, s.ea), BF16),
            vmem((s.ea, s.fb), F32),
            vmem((s.ea, s.fb), F32),
            vmem((2, s.ea // 2, s.fb), BF16),
            vmem((s.kh, 2, s.ea // 2, s.fb), BF16),
            vmem((s.nz, s.fb, s.fb), F32),
            vmem((s.nz, s.fb, s.fb), BF16),
            vmem((s.nz, s.fb, s.fb), BF16),
            vmem((s.nz, s.fb, s.fb), BF16),
            dma((17,)),
            dma((12,)),
            dma((4,)),
            dma((2, 4)),
            dma((4,)),
            dma,
            dma((5,)),
            dma((2,)),
            dma((2,)),
            dma((s.hops, CHUNKS)),
            dma((2,)),
            dma((2,)),
            dma((s.hops, CHUNKS)),
            dma((2,)),
            dma((2,)),
            dma((s.hops, 2)),
            dma((2,)),
            dma((2,)),
            dma((s.hops, 2)),
            dma((s.hops + 1,)),
            dma((s.hops + 1,)),
            dma((s.hops + 1,)),
            dma((s.hops + 1,)),
            dma((2,)),
        ],
        compiler_params=pltpu.CompilerParams(
            collective_id=0, has_side_effects=True, vmem_limit_bytes=VMEM_CAP
        ),
        cost_estimate=pl.CostEstimate(flops=60_000_000_000, bytes_accessed=16_000_000, transcendentals=0),
    )(features, grad_out, eigvecs.T, eigvals.reshape(s.nk, 1, s.ea), whiten.reshape(s.nz, s.fb, fb))


def solution(mesh):
    in_specs = (P("rows", "feat"), P("rows", "feat"), P("feat", "rows"), P(), P(None, "feat"))
    out_specs = P("rows", "feat")
    return jax.shard_map(local, mesh=mesh, in_specs=in_specs, out_specs=out_specs, check_vma=False)
```

```python
import functools

import jax
import jax.numpy as jnp
from jax import lax
from jax.experimental import pallas as pl
from jax.experimental.pallas import tpu as pltpu
from jax.sharding import PartitionSpec as P

MESH = pl.DeviceIdType.MESH
F32 = jnp.float32
BF16 = jnp.bfloat16
VMEM_CAP = 62 * 1024 * 1024
CHUNKS = 8
ROW_TILES = 2


class Dims:
    def __init__(self, rows, feat, tokens, d):
        self.nr, self.nz = rows, feat
        self.nk = rows // 2
        self.nx = {4: 2, 16: 4}[self.nk]
        self.ny = self.nk // self.nx
        self.kh = self.nk // 2
        self.d, self.dh = d, d // 2
        self.n = tokens
        self.tok = tokens // rows
        self.fb = d // feat
        self.fbh = self.fb // 2
        self.sr = self.fb // self.nk
        self.ea = d // self.nk
        self.er = d // rows
        self.hops = feat // 2

    def slot(self, src, g):
        dist = (g - src) % self.nz
        if dist == 0:
            return 0
        if dist == self.hops:
            return self.nz - 1
        return 2 * dist if dist < self.hops else 2 * (self.nz - dist) - 1


def where_am_i():
    r = lax.axis_index("rows")
    z = lax.axis_index("feat")
    return r, z, r // 2, lax.rem(r, 2)


def send(src, dst, ss, rs, r, z):
    copy = pltpu.make_async_remote_copy(
        src, dst, ss, rs, device_id={"rows": r, "feat": z}, device_id_type=MESH
    )
    copy.start()


def arrive(ref, sem):
    pltpu.make_async_copy(ref, ref, sem).wait()


def greet(s, r, z):
    barrier = pltpu.get_barrier_semaphore()

    def plane(t, _):
        pl.semaphore_signal(
            barrier, 1, device_id={"rows": lax.rem(r + t, s.nr), "feat": z}, device_id_type=MESH
        )
        return 0

    def line(t, _):
        pl.semaphore_signal(
            barrier, 1, device_id={"rows": r, "feat": lax.rem(z + t, s.nz)}, device_id_type=MESH
        )
        return 0

    lax.fori_loop(1, s.nr, plane, 0)
    lax.fori_loop(1, s.nz, line, 0)
    return lambda: pl.semaphore_wait(barrier, s.nr - 1 + s.nz - 1)


class Ring:
    def __init__(self, s, r, z, own, buf, cuts, ssem, hsem, rsem):
        self.s, self.r, self.z = s, r, z
        self.own, self.buf, self.cuts = own, buf, cuts
        self.ssem, self.hsem, self.rsem = ssem, hsem, rsem
        self.done = set()

    def new(self, h, qs):
        fresh = [q for q in qs if (h, q) not in self.done]
        self.done.update((h, q) for q in fresh)
        return fresh

    def block(self, way, h):
        nz = self.s.nz
        return lax.rem(self.z + (nz - h if way == 0 else h), nz)

    def rows(self, q):
        return pl.ds(*self.cuts[q])

    def start(self, way, h, q):
        s = self.s
        to = lax.rem(self.z + (1 if way == 0 else s.nz - 1), s.nz)
        blk = self.block(way, h - 1)
        src = self.own.at[self.rows(q)] if h == 1 else self.buf.at[blk, self.rows(q)]
        ss = self.hsem if h == s.hops else self.ssem
        send(src, self.buf.at[blk, self.rows(q)], ss.at[way], self.rsem.at[h - 1, q], self.r, to)

    def has(self, way, h, q):
        return h < self.s.hops or (q < len(self.cuts) // 2) == (way == 0)

    def begin(self, qs):
        for q in self.new(0, qs):
            for way in (0, 1):
                self.start(way, 1, q)

    def step(self, h, qs):
        for q in self.new(h, qs):
            ways = [way for way in (0, 1) if self.has(way, h, q)]
            both = pl.ds(0, len(ways) * self.cuts[q][1])
            arrive(self.buf.at[0, both], self.rsem.at[h - 1, q])
            for way in ways:
                if h < self.s.hops and self.has(way, h + 1, q):
                    self.start(way, h + 1, q)

    def drain(self):
        sizes = [size for _, size in self.cuts]
        half = len(sizes) // 2
        for way, far in ((0, sum(sizes[:half])), (1, sum(sizes[half:]))):
            near = self.buf.at[pl.ds(0, self.s.hops - 1), pl.ds(0, sum(sizes))]
            arrive(near, self.ssem.at[way])
            arrive(self.buf.at[0, pl.ds(0, far)], self.hsem.at[way])


def even(length, parts):
    return [(i * length // parts, length // parts) for i in range(parts)]


class Axis:
    def __init__(self, n, pos, device, z, block, part, ssem, rsem):
        self.n, self.pos, self.device, self.z = n, pos, device, z
        self.block, self.part, self.ssem, self.rsem = block, part, ssem, rsem
        self.right = lax.rem(pos + 1, n)
        self.left = lax.rem(pos + n - 1, n)
        self.far = lax.rem(pos + 2, n)

    def put(self, ref, sem, to):
        send(ref, ref, self.ssem, self.rsem.at[sem], self.device(to), self.z)

    def start(self):
        self.put(self.block(self.pos), 0, self.right)
        if self.n > 2:
            self.put(self.block(self.pos), 1, self.left)

    def forward(self):
        arrive(self.block(0), self.rsem.at[0])
        if self.n > 2:
            self.put(self.part(self.left, 0), 2, self.right)
            arrive(self.block(0), self.rsem.at[1])
            self.put(self.part(self.right, 1), 3, self.left)

    def finish(self):
        if self.n > 2:
            arrive(self.part(0, 0), self.rsem.at[2])
            arrive(self.part(0, 1), self.rsem.at[3])


def whole_kernel(
    s, x_hbm, g_hbm, v_hbm, e_hbm, w_hbm, out_ref,
    x_ref, g_ref, v_ref, e_ref, w_ref, ga, xa, grid, vv, pad, pad_in, tile, m_out, m_in, mean, xct, acc, kk_buf,
    cp, cp_in, part, part_in, c128, t1s, t1r, mt, sy_out, sy_in, t2p, t2d, t2s, t2g,
    sp, sp_out, sp_in, sens,
    ssem, rsem, asem, bsem, bfar, lsem, isem, gs, gh, gr, xs, xh, xr, vs, vh, vr, cs, ch, cr, ds_, dr_, rs_, rr_, zr_,
):
    r, z, k, c = where_am_i()
    y, x = k // s.nx, lax.rem(k, s.nx)
    mate = r + 1 - 2 * c
    first = c == 0
    a = jnp.where(first, x, y)
    b = jnp.where(first, y, x)
    half = k // s.kh
    mine = half == c
    kk = lax.rem(k, s.kh)
    every = range(CHUNKS)
    cuts = even(x_ref.shape[0], CHUNKS)
    early = 2 * s.hops - 3
    g_ring = Ring(s, r, z, g_ref, ga, cuts, gs, gh, gr)
    x_ring = Ring(s, r, z, xa.at[z], xa, cuts, xs, xh, xr)
    v_ring = Ring(s, r, z, grid.at[b, a, z], grid.at[b, a], even(s.fbh, 2), vs, vh, vr)
    early_cuts = [(0, (early + 1) // 2), ((early + 1) // 2, early // 2)]
    c_ring = Ring(s, r, z, c128.at[c, z], c128.at[c], early_cuts, cs, ch, cr)

    welcome = greet(s, r, z)
    inputs = (v_hbm, v_ref), (g_hbm, g_ref), (x_hbm, x_ref), (e_hbm, e_ref), (w_hbm, w_ref)
    loads = [
        pltpu.make_async_copy(src, dst, isem.at[i])
        for i, (src, dst) in enumerate(inputs)
    ]
    for load in loads:
        load.start()
    loads[0].wait()
    v = v_ref[...].T
    twice = jnp.concatenate([v, v], axis=1)
    lane_half = lax.broadcasted_iota(jnp.int32, twice.shape, 1) // s.er
    pad[...] = jnp.where(lane_half == c, twice, 0.0).astype(BF16)
    loads[1].wait()
    loads[2].wait()
    sum_x = jnp.sum(x_ref[...].astype(F32), axis=0, keepdims=True)
    sum_g = jnp.sum(g_ref[...].astype(F32), axis=0, keepdims=True)
    m_out[0] = jnp.concatenate([sum_x, sum_g], axis=1)
    m_in[r] = m_out[0]

    welcome()

    send(pad, pad_in, ssem.at[0], rsem.at[0], mate, z)
    g_ring.begin([0])

    def sums(t, _):
        send(m_out.at[0], m_in.at[r], ssem.at[1], rsem.at[1], lax.rem(r + t, s.nr), z)
        return 0

    lax.fori_loop(1, s.nr, sums, 0)
    arrive(pad_in, rsem.at[0])
    tile[...] = pad[...] + pad_in[...]
    grid[b, a, z] = tile[pl.ds(pl.multiple_of(c * s.fbh, s.fbh), s.fbh), :]

    v_ring.begin([0, 1])
    g_ring.begin([1, 2, 3])
    ga[z] = g_ref[...]

    loads[3].wait()
    s_row = jnp.broadcast_to(lax.rsqrt(e_ref[k]), (s.ea, s.ea)).T
    for j in range(s.kh):
        s_col = lax.rsqrt(e_ref[c * s.kh + j])
        both = s_row * s_col
        kk_buf[:, j * s.ea : (j + 1) * s.ea] = -(both * both) / (s_row + s_col)
    acc[...] = jnp.zeros_like(acc)
    loads[4].wait()
    v_ring.step(1, [0, 1])
    g_ring.begin([4, 5])

    arrive(m_in.at[pl.ds(0, s.nr - 1)], rsem.at[1])
    own_mean = jnp.sum(m_in[...], axis=0) / s.n
    mean[z] = own_mean

    def mean_up(t, _):
        send(mean.at[z], mean.at[z], ssem.at[3], rsem.at[3], r, lax.rem(z + t, s.nz))
        return 0

    lax.fori_loop(1, s.nz, mean_up, 0)
    if s.hops > 2:
        v_ring.step(2, [0, 1])
    g_ring.begin([6, 7])
    centered = (x_ref[...].astype(F32) - own_mean[:, : s.fb]).astype(BF16)
    xa[z] = centered
    xct[...] = centered.astype(F32).T.astype(BF16)
    col_sum = jnp.sum(xct[...].astype(F32), axis=1, keepdims=True)

    def gram(slot, blk):
        nu = mean[blk][:, s.fb :]
        prod = jnp.dot(xct[...], ga[blk], preferred_element_type=F32) - col_sum * nu
        cp[slot, 0] = prod[:, : s.fbh]
        cp[slot, 1] = prod[:, s.fbh :]

    def product(blk):
        nu = mean[blk][:, s.fb :]
        shifted = (ga[blk].astype(F32) - nu).astype(BF16)
        acc[...] += jnp.dot(shifted, w_ref[blk], preferred_element_type=F32)

    def round_of(h):
        if h == 0:
            return [(0, z)]
        if h == s.hops:
            return [(s.nz - 1, g_ring.block(0, h))]
        return [(2 * h - 1, g_ring.block(0, h)), (2 * h, g_ring.block(1, h))]

    def round_start(h):
        pairs = round_of(h)
        slots = pl.ds(pairs[0][0], len(pairs))
        for slot, blk in pairs:
            gram(slot, blk)
        send(cp.at[slots, 1 - c], cp_in.at[slots], ds_.at[h], dr_.at[h], mate, z)

    def round_scatter(h):
        pairs = round_of(h)
        slots = pl.ds(pairs[0][0], len(pairs))
        arrive(cp_in.at[slots], dr_.at[h])
        for slot, _ in pairs:
            both = cp[slot, c] + cp_in[slot]
            part[:, slot] = both.reshape(s.nk, s.sr, s.fbh).astype(BF16)

        def scatter(t, _):
            k2 = lax.rem(k + t, s.nk)
            send(part.at[k2, slots], part_in.at[k, slots], rs_.at[h], rr_.at[h], 2 * k2 + c, z)
            return 0

        lax.fori_loop(1, s.nk, scatter, 0)
        part_in[k, slots] = part[k, slots]

    def round_sum(hs):
        for h in hs:
            arrive(part_in.at[pl.ds(0, s.nk - 1), pl.ds(0, len(round_of(h)))], rr_.at[h])
        lo = round_of(hs[0])[0][0]
        n = round_of(hs[-1])[-1][0] + 1 - lo
        slots = pl.ds(lo, n)
        c128[c, z, slots] = jnp.sum(part_in[:, slots].astype(F32), axis=0).astype(BF16)

        return slots

    def round_lift(h, batch):
        slots = round_sum([h])

        def lift(t, _):
            send(
                c128.at[c, z, slots], c128.at[c, z, slots], ssem.at[9 + batch], zr_.at[batch],
                r, lax.rem(z + t, s.nz),
            )
            return 0

        lax.fori_loop(1, s.nz, lift, 0)

    assert s.nx == s.ny and s.nx in (2, 4)
    nzh = s.nz // 2

    def device(a2, b2):
        y2, x2 = jnp.where(first, b2, a2), jnp.where(first, a2, b2)
        return (y2 * s.nx + x2) * 2 + c

    axis_a = Axis(
        s.nx, a, lambda p: device(p, b), z, lambda p: grid.at[b, p],
        lambda p, i: grid.at[b, p, pl.ds(i * nzh, nzh)], ssem.at[4], asem,
    )
    b_right, b_left = lax.rem(b + 1, s.ny), lax.rem(b + s.ny - 1, s.ny)
    b_far = lax.rem(b + 2, s.ny)
    pieces = [a, axis_a.left] + ([axis_a.right, axis_a.far] if s.nx > 2 else [])

    def put_b(b2, piece, sem, to):
        ref = grid.at[b2, pieces[piece]]
        send(ref, ref, ssem.at[5], sem, device(a, to), z)

    def b_start(piece):
        put_b(b, piece, bsem.at[0, piece], b_right)
        if s.ny > 2:
            put_b(b, piece, bsem.at[1, piece], b_left)

    def b_forward():
        for piece in range(len(pieces)):
            arrive(grid.at[0, 0], bsem.at[0, piece])
            if s.ny > 2:
                if piece % 2 == 0:
                    put_b(b_left, piece, bfar.at[piece], b_right)
                arrive(grid.at[0, 0], bsem.at[1, piece])
                if piece % 2 == 1:
                    put_b(b_right, piece, bfar.at[piece], b_left)

    def b_finish():
        if s.ny > 2:
            for piece in range(len(pieces)):
                arrive(grid.at[0, 0], bfar.at[piece])

    def hand_out(b2):
        def each(a2, _):
            y2, x2 = jnp.where(first, b2, a2), jnp.where(first, a2, b2)
            to = y2 // (s.ny // 2)
            pos = lax.rem(y2, s.ny // 2) * s.nx + x2
            cols = pl.ds(pl.multiple_of(pos * s.ea, s.ea), s.ea)
            dst = vv.at[:, c, :, cols]

            @pl.when(to == c)
            def _():
                pltpu.make_async_copy(grid.at[b2, a2], dst, lsem).start()

            @pl.when(to != c)
            def _():
                send(grid.at[b2, a2], dst, ssem.at[6], rsem.at[6], mate, z)

            return 0

        lax.fori_loop(0, s.nx, each, 0)

    if s.hops > 3:
        v_ring.step(3, [0, 1])
    g_ring.step(1, every[:4])
    v_ring.step(s.hops, [0, 1])
    axis_a.start()
    b_start(0)
    g_ring.step(1, every[4:])
    arrive(mean.at[pl.ds(0, s.nz - 1)], rsem.at[3])
    round_start(0)
    g_ring.step(2, every[:3])
    axis_a.forward()
    b_start(1)
    if s.nx > 2:
        b_start(2)
    round_scatter(0)

    for h in range(1, s.hops):
        round_start(h)
        if h < s.hops - 1:
            g_ring.step(h + 1, every[:4])
        if h == 1:
            axis_a.finish()
            if s.nx > 2:
                b_start(3)
            hand_out(b)
        for _, blk in round_of(h - 1):
            product(blk)
        round_scatter(h)
        if h == s.hops - 1:
            round_sum(range(0, h))
            c_ring.begin([0, 1])
            x_ring.begin(every[:2])
            b_forward()
            hand_out(b_left)
            if s.ny > 2:
                hand_out(b_right)
        g_ring.step(h + 1, every)

    round_start(s.hops)
    if s.hops > 2:
        c_ring.step(1, [0, 1])
    x_ring.begin([2])
    round_scatter(s.hops)
    round_lift(s.hops - 1, 0)
    if s.hops > 2:
        c_ring.step(2, [0, 1])
    x_ring.begin([3, 4])
    for h in (s.hops - 1, s.hops):
        for _, blk in round_of(h):
            product(blk)
    round_lift(s.hops, 1)
    if s.hops > 2:
        c_ring.step(3, [0, 1])
    x_ring.begin(every)
    x_ring.step(1, every[:3])
    b_finish()
    if s.ny > 2:
        hand_out(b_far)

    c_ring.step(s.hops, [0, 1])
    arrive(c128.at[c, pl.ds(0, s.nz - 1), pl.ds(0, 2)], zr_.at[0])
    arrive(c128.at[c, pl.ds(0, s.nz - 1), pl.ds(0, 1)], zr_.at[1])
    send(c128.at[c], c128.at[c], ssem.at[12], rsem.at[7], mate, z)
    arrive(vv.at[:, c], lsem)
    arrive(vv.at[:, 1 - c], rsem.at[6])

    def cross_rows(h):
        bands = []
        for src in range(s.nz):
            bands.append(jnp.concatenate([c128[h, src, s.slot(src, g)] for g in range(s.nz)], axis=1))
        return jnp.concatenate(bands, axis=0)

    mt[...] = jnp.dot(
        cross_rows(c), vv[:, c].reshape(s.dh, s.dh), preferred_element_type=F32
    )
    arrive(c128.at[1 - c], rsem.at[7])
    other = cross_rows(1 - c)
    for t in range(s.kh // 2):
        pair = lax.rem(kk // 2 + t, s.kh // 2)
        cols = pl.ds(pl.multiple_of(pair * 2 * s.ea, 2 * s.ea), 2 * s.ea)
        t1 = mt[:, cols] + jnp.dot(
            other, vv[:, 1 - c, :, cols].reshape(s.dh, 2 * s.ea), preferred_element_type=F32
        )
        for i in range(2):
            j = pair * 2 + i
            k2 = c * s.kh + j
            t1s[j] = t1[:, i * s.ea : (i + 1) * s.ea].astype(BF16).reshape(s.nz, s.sr, s.ea)

            @pl.when(k2 != k)
            def _():
                send(t1s.at[j], t1r.at[:, k], ssem.at[7], rsem.at[8], 2 * k2 + c, z)

            send(t1s.at[j], t1r.at[:, k], ssem.at[8], rsem.at[8], 2 * k2 + 1 - c, z)

    x_ring.step(1, every)

    @pl.when(mine)
    def _():
        t1r[:, k] = t1s[kk]
        arrive(t1r.at[:, pl.ds(0, s.nk - 1)], rsem.at[8])
        arrive(t1s.at[pl.ds(0, s.kh - 1)], ssem.at[7])

    @pl.when(jnp.logical_not(mine))
    def _():
        arrive(t1r, rsem.at[8])
        arrive(t1s, ssem.at[7])

    left = t1r[...].reshape(s.d, s.ea).astype(F32).T.astype(BF16)
    mt[...] = jnp.dot(left, vv[...].reshape(s.d, s.dh), preferred_element_type=F32)
    for j in range(s.kh):
        sy_out[j] = mt[:, j * s.ea : (j + 1) * s.ea].T.astype(BF16)

    def mirror(t, _):
        j = lax.rem(kk + t, s.kh)
        k2 = c * s.kh + j

        @pl.when(k2 != k)
        def _():
            send(sy_out.at[j], sy_in.at[kk], ssem.at[13], rsem.at[9], 2 * k2 + half, z)

        return 0

    lax.fori_loop(0, s.kh, mirror, 0)
    x_ring.step(2, every[:4])

    @pl.when(mine)
    def _():
        sy_in[kk] = sy_out[kk]
        arrive(sy_in.at[pl.ds(0, s.kh - 1)], rsem.at[9])
        arrive(sy_out.at[pl.ds(0, s.kh - 1)], ssem.at[13])

    @pl.when(jnp.logical_not(mine))
    def _():
        arrive(sy_in, rsem.at[9])
        arrive(sy_out, ssem.at[13])

    total = jnp.zeros((s.ea, s.fb), F32)
    own_rows = vv.at[z]
    for j in range(s.kh):
        cols = slice(j * s.ea, (j + 1) * s.ea)
        rotated = 0.5 * (mt[:, cols] + sy_in[j].astype(F32))
        weighted = (kk_buf[:, cols] * rotated).astype(BF16)
        right = own_rows[:, :, cols].reshape(s.fb, s.ea)
        total += lax.dot_general(
            weighted, right, (((1,), (1,)), ((), ())), preferred_element_type=F32
        )
    t2p[...] = total
    send(t2p, t2d, ssem.at[14], rsem.at[10], mate, z)
    x_ring.step(2, every[4:])
    arrive(t2d, rsem.at[10])
    t2s[...] = (t2p[...] + t2d[...]).astype(BF16).reshape(t2s.shape)

    def spread(t, _):
        k2 = lax.rem(k + t, s.nk)
        send(t2s.at[c], t2g.at[kk, c], ssem.at[15], rsem.at[11], 2 * k2 + half, z)
        return 0

    lax.fori_loop(1, s.nk, spread, 0)
    x_ring.step(3, every)

    @pl.when(mine)
    def _():
        t2g[kk] = t2s[...]
        arrive(t2g.at[pl.ds(0, s.kh - 1)], rsem.at[11])

    @pl.when(jnp.logical_not(mine))
    def _():
        arrive(t2g, rsem.at[11])

    right2 = t2g[...].reshape(s.dh, s.fb)

    def back(q, _):
        two = pl.ds(2 * q, 2)
        left2 = vv[two].reshape(2 * s.fb, s.dh)
        prod = jnp.dot(left2, right2, preferred_element_type=F32) * (2.0 / s.n)
        prod = prod.reshape(2, s.fb, s.fb)
        sp[two] = prod
        sp_out[two] = prod.astype(BF16)
        send(sp_out.at[two], sp_in.at[two], ssem.at[16], bsem.at[0, q], mate, z)
        return 0

    lax.fori_loop(0, s.nz // 4, back, 0)
    lax.fori_loop(s.nz // 4, s.nz // 2, back, 0)
    for q in range(s.nz):
        if q % 2 == 0:
            arrive(sp_in.at[pl.ds(0, 2)], bsem.at[0, q // 2])
        sens[q] = (sp[q] + sp_in[q].astype(F32)).astype(BF16)

    far = x_ring.block(0, s.hops)
    tile_rows = x_ref.shape[0] // ROW_TILES

    def most(m, _):
        rows = pl.ds(pl.multiple_of(m * tile_rows, tile_rows), tile_rows)
        res = acc[rows, :]
        for q in range(s.nz):
            if q != s.hops:
                blk = lax.rem(z + q, s.nz)
                res += jnp.dot(xa[blk, rows, :], sens[blk], preferred_element_type=F32)
        acc[rows, :] = res
        return 0

    lax.fori_loop(0, ROW_TILES, most, 0)
    x_ring.step(s.hops, every)

    def last(m, _):
        rows = pl.ds(pl.multiple_of(m * tile_rows, tile_rows), tile_rows)
        res = acc[rows, :] + jnp.dot(xa[far, rows, :], sens[far], preferred_element_type=F32)
        out_ref[rows, :] = res.astype(BF16)
        return 0

    lax.fori_loop(0, ROW_TILES, last, 0)

    g_ring.drain()
    x_ring.drain()
    arrive(pad, ssem.at[0])
    arrive(m_in.at[pl.ds(0, s.nr - 1)], ssem.at[1])
    v_ring.drain()
    arrive(mean.at[pl.ds(0, s.nz - 1)], ssem.at[3])
    arrive(grid.at[0, pl.ds(0, s.nx - 1)], ssem.at[4])
    arrive(grid.at[pl.ds(0, s.ny - 1)], ssem.at[5])
    arrive(vv.at[:, c], ssem.at[6])
    arrive(t1s, ssem.at[8])
    c_ring.drain()
    arrive(c128.at[c, pl.ds(0, s.nz - 1), pl.ds(0, 2)], ssem.at[9])
    arrive(c128.at[c, pl.ds(0, s.nz - 1), pl.ds(0, 1)], ssem.at[10])
    arrive(c128.at[c], ssem.at[12])
    arrive(t2p, ssem.at[14])
    arrive(part.at[pl.ds(0, s.nk - 1)], ssem.at[15])
    arrive(sp_out, ssem.at[16])
    for h in range(s.hops + 1):
        n = len(round_of(h))
        arrive(cp_in.at[pl.ds(0, n)], ds_.at[h])
        arrive(part_in.at[pl.ds(0, s.nk - 1), pl.ds(0, n)], rs_.at[h])


def local(features, grad_out, eigvecs, eigvals, whiten):
    tok, fb = features.shape
    s = Dims(lax.axis_size("rows"), lax.axis_size("feat"), tok * lax.axis_size("rows"), whiten.shape[0])
    dma = pltpu.SemaphoreType.DMA
    vmem = pltpu.VMEM
    vm = pl.BlockSpec(memory_space=pltpu.VMEM)
    hbm = pl.BlockSpec(memory_space=pl.ANY)
    return pl.pallas_call(
        functools.partial(whole_kernel, s),
        name="whole",
        out_shape=pltpu.VMEM((tok, fb), BF16),
        in_specs=[hbm] * 5,
        out_specs=vm,
        scratch_shapes=[
            vmem((tok, fb), BF16),
            vmem((tok, fb), BF16),
            vmem((s.er, s.fb), F32),
            vmem((s.nk, 1, s.ea), F32),
            vmem((s.nz, s.fb, fb), BF16),
            vmem((s.nz, tok, fb), BF16),
            vmem((s.nz, tok, fb), BF16),
            vmem((s.ny, s.nx, s.nz, s.fbh, s.ea), BF16),
            vmem((s.nz, 2, s.fbh, s.dh), BF16),
            vmem((s.fb, s.ea), BF16),
            vmem((s.fb, s.ea), BF16),
            vmem((s.fb, s.ea), BF16),
            vmem((1, 1, 2 * s.fb), F32),
            vmem((s.nr, 1, 2 * s.fb), F32),
            vmem((s.nz, 1, 2 * s.fb), F32),
            vmem((fb, tok), BF16),
            vmem((tok, fb), F32),
            vmem((s.ea, s.dh), F32),
            vmem((s.nz, 2, s.fb, s.fbh), F32),
            vmem((s.nz, s.fb, s.fbh), F32),
            vmem((s.nk, s.nz, s.sr, s.fbh), BF16),
            vmem((s.nk, s.nz, s.sr, s.fbh), BF16),
            vmem((2, s.nz, s.nz, s.sr, s.fbh), BF16),
            vmem((s.kh, s.nz, s.sr, s.ea), BF16),
            vmem((s.nz, s.nk, s.sr, s.ea), BF16),
            vmem((s.ea, s.dh), F32),
            vmem((s.kh, s.ea, s.ea), BF16),
            vmem((s.kh, s.ea, s.ea), BF16),
            vmem((s.ea, s.fb), F32),
            vmem((s.ea, s.fb), F32),
            vmem((2, s.ea // 2, s.fb), BF16),
            vmem((s.kh, 2, s.ea // 2, s.fb), BF16),
            vmem((s.nz, s.fb, s.fb), F32),
            vmem((s.nz, s.fb, s.fb), BF16),
            vmem((s.nz, s.fb, s.fb), BF16),
            vmem((s.nz, s.fb, s.fb), BF16),
            dma((17,)),
            dma((12,)),
            dma((4,)),
            dma((2, 4)),
            dma((4,)),
            dma,
            dma((5,)),
            dma((2,)),
            dma((2,)),
            dma((s.hops, CHUNKS)),
            dma((2,)),
            dma((2,)),
            dma((s.hops, CHUNKS)),
            dma((2,)),
            dma((2,)),
            dma((s.hops, 2)),
            dma((2,)),
            dma((2,)),
            dma((s.hops, 2)),
            dma((s.hops + 1,)),
            dma((s.hops + 1,)),
            dma((s.hops + 1,)),
            dma((s.hops + 1,)),
            dma((2,)),
        ],
        compiler_params=pltpu.CompilerParams(
            collective_id=0, has_side_effects=True, vmem_limit_bytes=VMEM_CAP
        ),
        cost_estimate=pl.CostEstimate(flops=60_000_000_000, bytes_accessed=16_000_000, transcendentals=0),
    )(features, grad_out, eigvecs.T, eigvals.reshape(s.nk, 1, s.ea), whiten.reshape(s.nz, s.fb, fb))


def solution(mesh):
    in_specs = (P("rows", "feat"), P("rows", "feat"), P("feat", "rows"), P(), P(None, "feat"))
    out_specs = P("rows", "feat")
    return jax.shard_map(local, mesh=mesh, in_specs=in_specs, out_specs=out_specs, check_vma=False)
```

```python
import functools

import jax
import jax.numpy as jnp
from jax import lax
from jax.experimental import pallas as pl
from jax.experimental.pallas import tpu as pltpu
from jax.sharding import PartitionSpec as P

MESH = pl.DeviceIdType.MESH
F32 = jnp.float32
BF16 = jnp.bfloat16
VMEM_CAP = 62 * 1024 * 1024
CHUNKS = 8
ROW_TILES = 2


class Dims:
    def __init__(self, rows, feat, tokens, d):
        self.nr, self.nz = rows, feat
        self.nk = rows // 2
        self.nx = {4: 2, 16: 4}[self.nk]
        self.ny = self.nk // self.nx
        self.kh = self.nk // 2
        self.d, self.dh = d, d // 2
        self.n = tokens
        self.tok = tokens // rows
        self.fb = d // feat
        self.fbh = self.fb // 2
        self.sr = self.fb // self.nk
        self.ea = d // self.nk
        self.er = d // rows
        self.hops = feat // 2

    def slot(self, src, g):
        dist = (g - src) % self.nz
        if dist == 0:
            return 0
        if dist == self.hops:
            return self.nz - 1
        return 2 * dist if dist < self.hops else 2 * (self.nz - dist) - 1


def where_am_i():
    r = lax.axis_index("rows")
    z = lax.axis_index("feat")
    return r, z, r // 2, lax.rem(r, 2)


def send(src, dst, ss, rs, r, z):
    copy = pltpu.make_async_remote_copy(
        src, dst, ss, rs, device_id={"rows": r, "feat": z}, device_id_type=MESH
    )
    copy.start()


def arrive(ref, sem):
    pltpu.make_async_copy(ref, ref, sem).wait()


def greet(s, r, z):
    barrier = pltpu.get_barrier_semaphore()

    def plane(t, _):
        pl.semaphore_signal(
            barrier, 1, device_id={"rows": lax.rem(r + t, s.nr), "feat": z}, device_id_type=MESH
        )
        return 0

    def line(t, _):
        pl.semaphore_signal(
            barrier, 1, device_id={"rows": r, "feat": lax.rem(z + t, s.nz)}, device_id_type=MESH
        )
        return 0

    lax.fori_loop(1, s.nr, plane, 0)
    lax.fori_loop(1, s.nz, line, 0)
    return lambda: pl.semaphore_wait(barrier, s.nr - 1 + s.nz - 1)


class Ring:
    def __init__(self, s, r, z, own, buf, cuts, ssem, hsem, rsem):
        self.s, self.r, self.z = s, r, z
        self.own, self.buf, self.cuts = own, buf, cuts
        self.ssem, self.hsem, self.rsem = ssem, hsem, rsem
        self.done = set()

    def new(self, h, qs):
        fresh = [q for q in qs if (h, q) not in self.done]
        self.done.update((h, q) for q in fresh)
        return fresh

    def block(self, way, h):
        nz = self.s.nz
        return lax.rem(self.z + (nz - h if way == 0 else h), nz)

    def rows(self, q):
        return pl.ds(*self.cuts[q])

    def start(self, way, h, q):
        s = self.s
        to = lax.rem(self.z + (1 if way == 0 else s.nz - 1), s.nz)
        blk = self.block(way, h - 1)
        src = self.own.at[self.rows(q)] if h == 1 else self.buf.at[blk, self.rows(q)]
        ss = self.hsem if h == s.hops else self.ssem
        send(src, self.buf.at[blk, self.rows(q)], ss.at[way], self.rsem.at[h - 1, q], self.r, to)

    def has(self, way, h, q):
        return h < self.s.hops or (q < len(self.cuts) // 2) == (way == 0)

    def begin(self, qs):
        for q in self.new(0, qs):
            for way in (0, 1):
                self.start(way, 1, q)

    def step(self, h, qs):
        for q in self.new(h, qs):
            ways = [way for way in (0, 1) if self.has(way, h, q)]
            both = pl.ds(0, len(ways) * self.cuts[q][1])
            arrive(self.buf.at[0, both], self.rsem.at[h - 1, q])
            for way in ways:
                if h < self.s.hops and self.has(way, h + 1, q):
                    self.start(way, h + 1, q)

    def drain(self):
        sizes = [size for _, size in self.cuts]
        half = len(sizes) // 2
        for way, far in ((0, sum(sizes[:half])), (1, sum(sizes[half:]))):
            near = self.buf.at[pl.ds(0, self.s.hops - 1), pl.ds(0, sum(sizes))]
            arrive(near, self.ssem.at[way])
            arrive(self.buf.at[0, pl.ds(0, far)], self.hsem.at[way])


def even(length, parts):
    return [(i * length // parts, length // parts) for i in range(parts)]


class Axis:
    def __init__(self, n, pos, device, z, block, part, ssem, rsem):
        self.n, self.pos, self.device, self.z = n, pos, device, z
        self.block, self.part, self.ssem, self.rsem = block, part, ssem, rsem
        self.right = lax.rem(pos + 1, n)
        self.left = lax.rem(pos + n - 1, n)
        self.far = lax.rem(pos + 2, n)

    def put(self, ref, sem, to):
        send(ref, ref, self.ssem, self.rsem.at[sem], self.device(to), self.z)

    def start(self):
        self.put(self.block(self.pos), 0, self.right)
        if self.n > 2:
            self.put(self.block(self.pos), 1, self.left)

    def forward(self):
        arrive(self.block(0), self.rsem.at[0])
        if self.n > 2:
            self.put(self.part(self.left, 0), 2, self.right)
            arrive(self.block(0), self.rsem.at[1])
            self.put(self.part(self.right, 1), 3, self.left)

    def finish(self):
        if self.n > 2:
            arrive(self.part(0, 0), self.rsem.at[2])
            arrive(self.part(0, 1), self.rsem.at[3])


def whole_kernel(
    s, x_hbm, g_hbm, v_hbm, e_hbm, w_hbm, out_ref,
    x_ref, g_ref, v_ref, e_ref, w_ref, ga, xa, grid, vv, pad, pad_in, tile, m_out, m_in, mean, xct, acc, kk_buf,
    cp, cp_in, part, part_in, c128, t1s, t1r, mt, sy_out, sy_in, t2p, t2d, t2s, t2g,
    sp, sp_out, sp_in, sens,
    ssem, rsem, asem, bsem, bfar, lsem, isem, gs, gh, gr, xs, xh, xr, vs, vh, vr, cs, ch, cr, ds_, dr_, rs_, rr_, zr_,
):
    r, z, k, c = where_am_i()
    y, x = k // s.nx, lax.rem(k, s.nx)
    mate = r + 1 - 2 * c
    first = c == 0
    a = jnp.where(first, x, y)
    b = jnp.where(first, y, x)
    half = k // s.kh
    mine = half == c
    kk = lax.rem(k, s.kh)
    every = range(CHUNKS)
    cuts = even(x_ref.shape[0], CHUNKS)
    early = 2 * s.hops - 3
    g_ring = Ring(s, r, z, g_ref, ga, cuts, gs, gh, gr)
    x_ring = Ring(s, r, z, xa.at[z], xa, cuts, xs, xh, xr)
    v_ring = Ring(s, r, z, grid.at[b, a, z], grid.at[b, a], even(s.fbh, 2), vs, vh, vr)
    early_cuts = [(0, (early + 1) // 2), ((early + 1) // 2, early // 2)]
    c_ring = Ring(s, r, z, c128.at[c, z], c128.at[c], early_cuts, cs, ch, cr)

    welcome = greet(s, r, z)
    inputs = (v_hbm, v_ref), (g_hbm, g_ref), (x_hbm, x_ref), (e_hbm, e_ref), (w_hbm, w_ref)
    loads = [
        pltpu.make_async_copy(src, dst, isem.at[i])
        for i, (src, dst) in enumerate(inputs)
    ]
    for load in loads:
        load.start()
    loads[0].wait()
    v = v_ref[...].T
    twice = jnp.concatenate([v, v], axis=1)
    lane_half = lax.broadcasted_iota(jnp.int32, twice.shape, 1) // s.er
    pad[...] = jnp.where(lane_half == c, twice, 0.0).astype(BF16)
    loads[1].wait()
    loads[2].wait()
    sum_x = jnp.sum(x_ref[...].astype(F32), axis=0, keepdims=True)
    sum_g = jnp.sum(g_ref[...].astype(F32), axis=0, keepdims=True)
    m_out[0] = jnp.concatenate([sum_x, sum_g], axis=1)
    m_in[r] = m_out[0]

    welcome()

    send(pad, pad_in, ssem.at[0], rsem.at[0], mate, z)
    g_ring.begin([0])

    def sums(t, _):
        send(m_out.at[0], m_in.at[r], ssem.at[1], rsem.at[1], lax.rem(r + t, s.nr), z)
        return 0

    lax.fori_loop(1, s.nr, sums, 0)
    arrive(pad_in, rsem.at[0])
    tile[...] = pad[...] + pad_in[...]
    grid[b, a, z] = tile[pl.ds(pl.multiple_of(c * s.fbh, s.fbh), s.fbh), :]

    v_ring.begin([0, 1])
    g_ring.begin([1, 2, 3])
    ga[z] = g_ref[...]

    loads[3].wait()
    s_row = jnp.broadcast_to(lax.rsqrt(e_ref[k]), (s.ea, s.ea)).T
    for j in range(s.kh):
        s_col = lax.rsqrt(e_ref[c * s.kh + j])
        both = s_row * s_col
        kk_buf[:, j * s.ea : (j + 1) * s.ea] = -(both * both) / (s_row + s_col)
    acc[...] = jnp.zeros_like(acc)
    loads[4].wait()
    v_ring.step(1, [0, 1])
    g_ring.begin([4, 5])

    arrive(m_in.at[pl.ds(0, s.nr - 1)], rsem.at[1])
    own_mean = jnp.sum(m_in[...], axis=0) / s.n
    mean[z] = own_mean

    def mean_up(t, _):
        send(mean.at[z], mean.at[z], ssem.at[3], rsem.at[3], r, lax.rem(z + t, s.nz))
        return 0

    lax.fori_loop(1, s.nz, mean_up, 0)
    if s.hops > 2:
        v_ring.step(2, [0, 1])
    g_ring.begin([6, 7])
    centered = (x_ref[...].astype(F32) - own_mean[:, : s.fb]).astype(BF16)
    xa[z] = centered
    xct[...] = centered.astype(F32).T.astype(BF16)
    col_sum = jnp.sum(xct[...].astype(F32), axis=1, keepdims=True)

    def gram(slot, blk):
        nu = mean[blk][:, s.fb :]
        prod = jnp.dot(xct[...], ga[blk], preferred_element_type=F32) - col_sum * nu
        cp[slot, 0] = prod[:, : s.fbh]
        cp[slot, 1] = prod[:, s.fbh :]

    def product(blk):
        nu = mean[blk][:, s.fb :]
        shifted = (ga[blk].astype(F32) - nu).astype(BF16)
        acc[...] += jnp.dot(shifted, w_ref[blk], preferred_element_type=F32)

    def round_of(h):
        if h == 0:
            return [(0, z)]
        if h == s.hops:
            return [(s.nz - 1, g_ring.block(0, h))]
        return [(2 * h - 1, g_ring.block(0, h)), (2 * h, g_ring.block(1, h))]

    def round_start(h):
        pairs = round_of(h)
        slots = pl.ds(pairs[0][0], len(pairs))
        for slot, blk in pairs:
            gram(slot, blk)
        send(cp.at[slots, 1 - c], cp_in.at[slots], ds_.at[h], dr_.at[h], mate, z)

    def round_scatter(h):
        pairs = round_of(h)
        slots = pl.ds(pairs[0][0], len(pairs))
        arrive(cp_in.at[slots], dr_.at[h])
        for slot, _ in pairs:
            both = cp[slot, c] + cp_in[slot]
            part[:, slot] = both.reshape(s.nk, s.sr, s.fbh).astype(BF16)

        def scatter(t, _):
            k2 = lax.rem(k + t, s.nk)
            send(part.at[k2, slots], part_in.at[k, slots], rs_.at[h], rr_.at[h], 2 * k2 + c, z)
            return 0

        lax.fori_loop(1, s.nk, scatter, 0)
        part_in[k, slots] = part[k, slots]

    def round_sum(hs):
        for h in hs:
            arrive(part_in.at[pl.ds(0, s.nk - 1), pl.ds(0, len(round_of(h)))], rr_.at[h])
        lo = round_of(hs[0])[0][0]
        n = round_of(hs[-1])[-1][0] + 1 - lo
        slots = pl.ds(lo, n)
        c128[c, z, slots] = jnp.sum(part_in[:, slots].astype(F32), axis=0).astype(BF16)

        return slots

    def round_lift(h, batch):
        slots = round_sum([h])

        def lift(t, _):
            send(
                c128.at[c, z, slots], c128.at[c, z, slots], ssem.at[9 + batch], zr_.at[batch],
                r, lax.rem(z + t, s.nz),
            )
            return 0

        lax.fori_loop(1, s.nz, lift, 0)

    assert s.nx == s.ny and s.nx in (2, 4)
    nzh = s.nz // 2

    def device(a2, b2):
        y2, x2 = jnp.where(first, b2, a2), jnp.where(first, a2, b2)
        return (y2 * s.nx + x2) * 2 + c

    axis_a = Axis(
        s.nx, a, lambda p: device(p, b), z, lambda p: grid.at[b, p],
        lambda p, i: grid.at[b, p, pl.ds(i * nzh, nzh)], ssem.at[4], asem,
    )
    b_right, b_left = lax.rem(b + 1, s.ny), lax.rem(b + s.ny - 1, s.ny)
    b_far = lax.rem(b + 2, s.ny)
    pieces = [a, axis_a.left] + ([axis_a.right, axis_a.far] if s.nx > 2 else [])

    def put_b(b2, piece, sem, to):
        ref = grid.at[b2, pieces[piece]]
        send(ref, ref, ssem.at[5], sem, device(a, to), z)

    def b_start(piece):
        put_b(b, piece, bsem.at[0, piece], b_right)
        if s.ny > 2:
            put_b(b, piece, bsem.at[1, piece], b_left)

    def b_forward():
        for piece in range(len(pieces)):
            arrive(grid.at[0, 0], bsem.at[0, piece])
            if s.ny > 2:
                if piece % 2 == 0:
                    put_b(b_left, piece, bfar.at[piece], b_right)
                arrive(grid.at[0, 0], bsem.at[1, piece])
                if piece % 2 == 1:
                    put_b(b_right, piece, bfar.at[piece], b_left)

    def b_finish():
        if s.ny > 2:
            for piece in range(len(pieces)):
                arrive(grid.at[0, 0], bfar.at[piece])

    def hand_out(b2):
        def each(a2, _):
            y2, x2 = jnp.where(first, b2, a2), jnp.where(first, a2, b2)
            to = y2 // (s.ny // 2)
            pos = lax.rem(y2, s.ny // 2) * s.nx + x2
            cols = pl.ds(pl.multiple_of(pos * s.ea, s.ea), s.ea)
            dst = vv.at[:, c, :, cols]

            @pl.when(to == c)
            def _():
                pltpu.make_async_copy(grid.at[b2, a2], dst, lsem).start()

            @pl.when(to != c)
            def _():
                send(grid.at[b2, a2], dst, ssem.at[6], rsem.at[6], mate, z)

            return 0

        lax.fori_loop(0, s.nx, each, 0)

    if s.hops > 3:
        v_ring.step(3, [0, 1])
    g_ring.step(1, every[:4])
    v_ring.step(s.hops, [0, 1])
    axis_a.start()
    b_start(0)
    g_ring.step(1, every[4:])
    arrive(mean.at[pl.ds(0, s.nz - 1)], rsem.at[3])
    round_start(0)
    g_ring.step(2, every[:3])
    axis_a.forward()
    b_start(1)
    if s.nx > 2:
        b_start(2)
    round_scatter(0)

    for h in range(1, s.hops):
        round_start(h)
        if h < s.hops - 1:
            g_ring.step(h + 1, every[:4])
        if h == 1:
            axis_a.finish()
            if s.nx > 2:
                b_start(3)
            hand_out(b)
        for _, blk in round_of(h - 1):
            product(blk)
        round_scatter(h)
        if h == s.hops - 1:
            round_sum(range(0, h))
            c_ring.begin([0, 1])
            x_ring.begin(every[:2])
            b_forward()
            hand_out(b_left)
            if s.ny > 2:
                hand_out(b_right)
        g_ring.step(h + 1, every)

    round_start(s.hops)
    if s.hops > 2:
        c_ring.step(1, [0, 1])
    x_ring.begin([2])
    round_scatter(s.hops)
    round_lift(s.hops - 1, 0)
    if s.hops > 2:
        c_ring.step(2, [0, 1])
    x_ring.begin([3, 4])
    for h in (s.hops - 1, s.hops):
        for _, blk in round_of(h):
            product(blk)
    round_lift(s.hops, 1)
    if s.hops > 2:
        c_ring.step(3, [0, 1])
    x_ring.begin(every)
    x_ring.step(1, every[:3])
    b_finish()
    if s.ny > 2:
        hand_out(b_far)

    c_ring.step(s.hops, [0, 1])
    arrive(c128.at[c, pl.ds(0, s.nz - 1), pl.ds(0, 2)], zr_.at[0])
    arrive(c128.at[c, pl.ds(0, s.nz - 1), pl.ds(0, 1)], zr_.at[1])
    send(c128.at[c], c128.at[c], ssem.at[12], rsem.at[7], mate, z)
    arrive(vv.at[:, c], lsem)
    arrive(vv.at[:, 1 - c], rsem.at[6])

    def cross_rows(h):
        bands = []
        for src in range(s.nz):
            bands.append(jnp.concatenate([c128[h, src, s.slot(src, g)] for g in range(s.nz)], axis=1))
        return jnp.concatenate(bands, axis=0)

    mt[...] = jnp.dot(
        cross_rows(c), vv[:, c].reshape(s.dh, s.dh), preferred_element_type=F32
    )
    arrive(c128.at[1 - c], rsem.at[7])
    other = cross_rows(1 - c)
    for t in range(s.kh // 2):
        pair = lax.rem(kk // 2 + t, s.kh // 2)
        cols = pl.ds(pl.multiple_of(pair * 2 * s.ea, 2 * s.ea), 2 * s.ea)
        t1 = mt[:, cols] + jnp.dot(
            other, vv[:, 1 - c, :, cols].reshape(s.dh, 2 * s.ea), preferred_element_type=F32
        )
        for i in range(2):
            j = pair * 2 + i
            k2 = c * s.kh + j
            t1s[j] = t1[:, i * s.ea : (i + 1) * s.ea].astype(BF16).reshape(s.nz, s.sr, s.ea)

            @pl.when(k2 != k)
            def _():
                send(t1s.at[j], t1r.at[:, k], ssem.at[7], rsem.at[8], 2 * k2 + c, z)

            send(t1s.at[j], t1r.at[:, k], ssem.at[8], rsem.at[8], 2 * k2 + 1 - c, z)

    x_ring.step(1, every)

    @pl.when(mine)
    def _():
        t1r[:, k] = t1s[kk]
        arrive(t1r.at[:, pl.ds(0, s.nk - 1)], rsem.at[8])
        arrive(t1s.at[pl.ds(0, s.kh - 1)], ssem.at[7])

    @pl.when(jnp.logical_not(mine))
    def _():
        arrive(t1r, rsem.at[8])
        arrive(t1s, ssem.at[7])

    left = t1r[...].reshape(s.d, s.ea).astype(F32).T.astype(BF16)
    mt[...] = jnp.dot(left, vv[...].reshape(s.d, s.dh), preferred_element_type=F32)
    for j in range(s.kh):
        sy_out[j] = mt[:, j * s.ea : (j + 1) * s.ea].T.astype(BF16)

    def mirror(t, _):
        j = lax.rem(kk + t, s.kh)
        k2 = c * s.kh + j

        @pl.when(k2 != k)
        def _():
            send(sy_out.at[j], sy_in.at[kk], ssem.at[13], rsem.at[9], 2 * k2 + half, z)

        return 0

    lax.fori_loop(0, s.kh, mirror, 0)
    x_ring.step(2, every[:4])

    @pl.when(mine)
    def _():
        sy_in[kk] = sy_out[kk]
        arrive(sy_in.at[pl.ds(0, s.kh - 1)], rsem.at[9])
        arrive(sy_out.at[pl.ds(0, s.kh - 1)], ssem.at[13])

    @pl.when(jnp.logical_not(mine))
    def _():
        arrive(sy_in, rsem.at[9])
        arrive(sy_out, ssem.at[13])

    total = jnp.zeros((s.ea, s.fb), F32)
    own_rows = vv.at[z]
    for j in range(s.kh):
        cols = slice(j * s.ea, (j + 1) * s.ea)
        rotated = 0.5 * (mt[:, cols] + sy_in[j].astype(F32))
        weighted = (kk_buf[:, cols] * rotated).astype(BF16)
        right = own_rows[:, :, cols].reshape(s.fb, s.ea)
        total += lax.dot_general(
            weighted, right, (((1,), (1,)), ((), ())), preferred_element_type=F32
        )
    t2p[...] = total
    send(t2p, t2d, ssem.at[14], rsem.at[10], mate, z)
    x_ring.step(2, every[4:])
    arrive(t2d, rsem.at[10])
    t2s[...] = (t2p[...] + t2d[...]).astype(BF16).reshape(t2s.shape)

    steps = [(dy, dx) for dy in range(s.ny) for dx in range(s.nx) if dy or dx]
    steps.sort(key=lambda o: -min(o[0], s.ny - o[0]) - min(o[1], s.nx - o[1]))
    for dy, dx in steps:
        k2 = lax.rem(y + dy, s.ny) * s.nx + lax.rem(x + dx, s.nx)
        send(t2s.at[c], t2g.at[kk, c], ssem.at[15], rsem.at[11], 2 * k2 + half, z)

    x_ring.step(3, every)

    @pl.when(mine)
    def _():
        t2g[kk] = t2s[...]
        arrive(t2g.at[pl.ds(0, s.kh - 1)], rsem.at[11])

    @pl.when(jnp.logical_not(mine))
    def _():
        arrive(t2g, rsem.at[11])

    right2 = t2g[...].reshape(s.dh, s.fb)

    def back(q, _):
        two = pl.ds(2 * q, 2)
        left2 = vv[two].reshape(2 * s.fb, s.dh)
        prod = jnp.dot(left2, right2, preferred_element_type=F32) * (2.0 / s.n)
        prod = prod.reshape(2, s.fb, s.fb)
        sp[two] = prod
        sp_out[two] = prod.astype(BF16)
        send(sp_out.at[two], sp_in.at[two], ssem.at[16], bsem.at[0, q], mate, z)
        return 0

    lax.fori_loop(0, s.nz // 4, back, 0)
    lax.fori_loop(s.nz // 4, s.nz // 2, back, 0)
    for q in range(s.nz):
        if q % 2 == 0:
            arrive(sp_in.at[pl.ds(0, 2)], bsem.at[0, q // 2])
        sens[q] = (sp[q] + sp_in[q].astype(F32)).astype(BF16)

    far = x_ring.block(0, s.hops)
    tile_rows = x_ref.shape[0] // ROW_TILES

    def most(m, _):
        rows = pl.ds(pl.multiple_of(m * tile_rows, tile_rows), tile_rows)
        res = acc[rows, :]
        for q in range(s.nz):
            if q != s.hops:
                blk = lax.rem(z + q, s.nz)
                res += jnp.dot(xa[blk, rows, :], sens[blk], preferred_element_type=F32)
        acc[rows, :] = res
        return 0

    lax.fori_loop(0, ROW_TILES, most, 0)
    x_ring.step(s.hops, every)

    def last(m, _):
        rows = pl.ds(pl.multiple_of(m * tile_rows, tile_rows), tile_rows)
        res = acc[rows, :] + jnp.dot(xa[far, rows, :], sens[far], preferred_element_type=F32)
        out_ref[rows, :] = res.astype(BF16)
        return 0

    lax.fori_loop(0, ROW_TILES, last, 0)

    g_ring.drain()
    x_ring.drain()
    arrive(pad, ssem.at[0])
    arrive(m_in.at[pl.ds(0, s.nr - 1)], ssem.at[1])
    v_ring.drain()
    arrive(mean.at[pl.ds(0, s.nz - 1)], ssem.at[3])
    arrive(grid.at[0, pl.ds(0, s.nx - 1)], ssem.at[4])
    arrive(grid.at[pl.ds(0, s.ny - 1)], ssem.at[5])
    arrive(vv.at[:, c], ssem.at[6])
    arrive(t1s, ssem.at[8])
    c_ring.drain()
    arrive(c128.at[c, pl.ds(0, s.nz - 1), pl.ds(0, 2)], ssem.at[9])
    arrive(c128.at[c, pl.ds(0, s.nz - 1), pl.ds(0, 1)], ssem.at[10])
    arrive(c128.at[c], ssem.at[12])
    arrive(t2p, ssem.at[14])
    arrive(part.at[pl.ds(0, s.nk - 1)], ssem.at[15])
    arrive(sp_out, ssem.at[16])
    for h in range(s.hops + 1):
        n = len(round_of(h))
        arrive(cp_in.at[pl.ds(0, n)], ds_.at[h])
        arrive(part_in.at[pl.ds(0, s.nk - 1), pl.ds(0, n)], rs_.at[h])


def local(features, grad_out, eigvecs, eigvals, whiten):
    tok, fb = features.shape
    s = Dims(lax.axis_size("rows"), lax.axis_size("feat"), tok * lax.axis_size("rows"), whiten.shape[0])
    dma = pltpu.SemaphoreType.DMA
    vmem = pltpu.VMEM
    vm = pl.BlockSpec(memory_space=pltpu.VMEM)
    hbm = pl.BlockSpec(memory_space=pl.ANY)
    return pl.pallas_call(
        functools.partial(whole_kernel, s),
        name="whole",
        out_shape=pltpu.VMEM((tok, fb), BF16),
        in_specs=[hbm] * 5,
        out_specs=vm,
        scratch_shapes=[
            vmem((tok, fb), BF16),
            vmem((tok, fb), BF16),
            vmem((s.er, s.fb), F32),
            vmem((s.nk, 1, s.ea), F32),
            vmem((s.nz, s.fb, fb), BF16),
            vmem((s.nz, tok, fb), BF16),
            vmem((s.nz, tok, fb), BF16),
            vmem((s.ny, s.nx, s.nz, s.fbh, s.ea), BF16),
            vmem((s.nz, 2, s.fbh, s.dh), BF16),
            vmem((s.fb, s.ea), BF16),
            vmem((s.fb, s.ea), BF16),
            vmem((s.fb, s.ea), BF16),
            vmem((1, 1, 2 * s.fb), F32),
            vmem((s.nr, 1, 2 * s.fb), F32),
            vmem((s.nz, 1, 2 * s.fb), F32),
            vmem((fb, tok), BF16),
            vmem((tok, fb), F32),
            vmem((s.ea, s.dh), F32),
            vmem((s.nz, 2, s.fb, s.fbh), F32),
            vmem((s.nz, s.fb, s.fbh), F32),
            vmem((s.nk, s.nz, s.sr, s.fbh), BF16),
            vmem((s.nk, s.nz, s.sr, s.fbh), BF16),
            vmem((2, s.nz, s.nz, s.sr, s.fbh), BF16),
            vmem((s.kh, s.nz, s.sr, s.ea), BF16),
            vmem((s.nz, s.nk, s.sr, s.ea), BF16),
            vmem((s.ea, s.dh), F32),
            vmem((s.kh, s.ea, s.ea), BF16),
            vmem((s.kh, s.ea, s.ea), BF16),
            vmem((s.ea, s.fb), F32),
            vmem((s.ea, s.fb), F32),
            vmem((2, s.ea // 2, s.fb), BF16),
            vmem((s.kh, 2, s.ea // 2, s.fb), BF16),
            vmem((s.nz, s.fb, s.fb), F32),
            vmem((s.nz, s.fb, s.fb), BF16),
            vmem((s.nz, s.fb, s.fb), BF16),
            vmem((s.nz, s.fb, s.fb), BF16),
            dma((17,)),
            dma((12,)),
            dma((4,)),
            dma((2, 4)),
            dma((4,)),
            dma,
            dma((5,)),
            dma((2,)),
            dma((2,)),
            dma((s.hops, CHUNKS)),
            dma((2,)),
            dma((2,)),
            dma((s.hops, CHUNKS)),
            dma((2,)),
            dma((2,)),
            dma((s.hops, 2)),
            dma((2,)),
            dma((2,)),
            dma((s.hops, 2)),
            dma((s.hops + 1,)),
            dma((s.hops + 1,)),
            dma((s.hops + 1,)),
            dma((s.hops + 1,)),
            dma((2,)),
        ],
        compiler_params=pltpu.CompilerParams(
            collective_id=0, has_side_effects=True, vmem_limit_bytes=VMEM_CAP
        ),
        cost_estimate=pl.CostEstimate(flops=60_000_000_000, bytes_accessed=16_000_000, transcendentals=0),
    )(features, grad_out, eigvecs.T, eigvals.reshape(s.nk, 1, s.ea), whiten.reshape(s.nz, s.fb, fb))


def solution(mesh):
    in_specs = (P("rows", "feat"), P("rows", "feat"), P("feat", "rows"), P(), P(None, "feat"))
    out_specs = P("rows", "feat")
    return jax.shard_map(local, mesh=mesh, in_specs=in_specs, out_specs=out_specs, check_vma=False)
```
